32 devices in a mesh: wide: 8 (over y, x, core), head: 4 (over z).
Axes of the slice: x: 2, y: 2, z: 4, core: 2. Of those that a mesh axis runs over, the one named last changes fastest.
Arguments:
- tokens: bfloat16 [16384, 1024], P(('wide', 'head')), may hold values from -6 to 6
- cotangent: bfloat16 [16384, 1024], P(('wide', 'head')), may hold values from -6 to 6
- w_query: bfloat16 [1024, 1024], P('wide', 'head'), may hold values from -0.25 to 0.25
- w_key: bfloat16 [1024, 1024], P('wide', 'head'), may hold values from -0.25 to 0.25
- w_value: bfloat16 [1024, 1024], P('wide', 'head'), may hold values from -0.1875 to 0.1875
- w_out: bfloat16 [1024, 1024], P('head', 'wide'), may hold values from -0.1875 to 0.1875
- w_up: bfloat16 [1024, 4096], P('wide', 'head'), may hold values from -0.1875 to 0.1875
- w_down: bfloat16 [4096, 1024], P('head', 'wide'), may hold values from -0.09375 to 0.09375
- norm_gain: float32 [4, 1024], replicated, may hold values from 0.25 to 1.75
- norm_bias: float32 [4, 1024], replicated, may hold values from -3 to 3
Outputs:
- block_out: bfloat16 [16384, 1024], P(('wide', 'head'))
- input_grad: float32 [16384, 1024], P(('wide', 'head'))
- grad_query: float32 [1024, 1024], P('wide', 'head')
- grad_key: float32 [1024, 1024], P('wide', 'head')
- grad_value: float32 [1024, 1024], P('wide', 'head')
- grad_out: float32 [1024, 1024], P('head', 'wide')
- grad_up: float32 [1024, 4096], P('wide', 'head')
- grad_down: float32 [4096, 1024], P('head', 'wide')
- gain_grad: float32 [4, 1024], replicated
- bias_grad: float32 [4, 1024], replicated
The draws below stay inside these ranges and needn't reach their ends.
All inputs are finite; a program needn't handle non-finite values.
Results may differ from the reference program's by a relative error of at most 0.015.
Values may be sent and summed in bfloat16 or wider, within the bound.
No kernel may reach another device: no remote copies, remote signals or barrier semaphores. Data moves between devices by JAX's collectives and lax.ppermute only.
A program may use at most 192 MiB of HBM per device.

```python
import math
import jax
import jax.numpy as jnp
from jax import lax

D = 1024
HEADS = 16
HD = 64
FF = 4096
SEQ = 2048
SEQS = 8
TOKENS = 16384


def spiked(values, key, source, target, parts, factor):
    def block_of(dim):
        return (jnp.arange(values.shape[dim]) // (values.shape[dim] // parts)).reshape((-1,) + (1,) * (values.ndim - 1 - dim))

    first = jax.random.permutation(key, parts)[block_of(target)]
    second = (block_of(target) + parts // 2) % parts
    return jnp.where((block_of(source) == first) | (block_of(source) == second), factor * values, values)


def levels(own_key, extent, cuts, smallest, high):
    level, own = 1.0, jax.random.fold_in(own_key, 6)
    for axis_at, parts in cuts:
        steps = jnp.exp(jax.random.uniform(jax.random.fold_in(own, axis_at), (parts,), jnp.float32, smallest / len(cuts), high / len(cuts)))
        level = level * jnp.repeat(steps, extent[axis_at] // parts).reshape([-1 if axis == axis_at else 1 for axis in range(len(extent))])
    return level


def scatter_about(key, shape, width, most, split=(), held_as=jnp.bfloat16):
    loudness = levels(key, shape, split, -0.22, 0.18) if split else 1.0
    array = jax.random.normal(key, shape, jnp.float32) * width * loudness
    return jnp.minimum(jnp.maximum(array, -most), most).astype(held_as)


def gaussian_with(stream_key, shape, scale, reach, cuts, heavy, kind=jnp.bfloat16):
    values = scale * jax.random.normal(stream_key, shape, jnp.float32)
    if cuts:
        values = values * levels(stream_key, shape, cuts, -0.22, 0.18)
    return jnp.clip(spiked(values, jax.random.fold_in(stream_key, 3), *heavy), -reach, reach).astype(kind)


def setup_inputs(seed: int = 0) -> dict:
    keys = jax.random.split(jax.random.key(seed), 11)
    return {
        "tokens": scatter_about(keys[0], (TOKENS, D), 1.0, 6.0, ((0, 32),)),
        "cotangent": gaussian_with(keys[1], (TOKENS, D), 1.0, 6.0, ((0, 32),), (0, 1, 32, 2.75)),
        "w_query": scatter_about(keys[2], (D, D), (D // 2) ** -0.5, 0.25, ((0, 8), (1, 4))),
        "w_key": scatter_about(keys[3], (D, D), (D // 2) ** -0.5, 0.25, ((0, 8), (1, 4))),
        "w_value": scatter_about(keys[4], (D, D), D ** -0.5, 0.1875, ((0, 8), (1, 4))),
        "w_out": scatter_about(keys[5], (D, D), D ** -0.5, 0.1875, ((0, 4), (1, 8))),
        "w_up": scatter_about(keys[6], (D, FF), D ** -0.5, 0.1875, ((0, 8), (1, 4))),
        "w_down": scatter_about(keys[7], (FF, D), FF ** -0.5, 0.09375, ((0, 4), (1, 8))),
        "norm_gain": jnp.clip(1.0 + 0.15 * jax.random.normal(keys[8], (4, D), jnp.float32), 0.25, 1.75),
        "norm_bias": scatter_about(keys[9], (4, D), 0.3, 3.0, (), jnp.float32),
    }


EPS = 1e-05

@jax.custom_vjp
def low(v):
    return lax.optimization_barrier(v.astype(jnp.bfloat16)).astype(jnp.float32)

@jax.custom_vjp
def low_back(v):
    return v

def low_keep(v):
    return (low(v), None)

def low_pass(kept, grad):
    return (grad,)

def back_keep(v):
    return (v, None)

def back_low(kept, grad):
    return (low(grad),)
low.defvjp(low_keep, low_pass)
low_back.defvjp(back_keep, back_low)

def layer_norm(values, gain, bias):
    average = lax.optimization_barrier(jnp.mean(values, axis=-1, keepdims=True))
    centred = values - average
    inverse = lax.rsqrt(lax.optimization_barrier(jnp.mean(centred * centred, axis=-1, keepdims=True)) + EPS)
    return centred * inverse * gain + bias

def both_round(values):
    return low(low_back(values))

def product(left_op, right_op):
    return jnp.dot(left_op, right_op, precision=lax.Precision.HIGHEST)

def attention(queries, key_rows, value_rows):
    length = queries.shape[0]
    block_rows = min(512, length)
    count_blocks = length // block_rows
    score_scale = 1.0 / math.sqrt(HD)
    query_blocks = queries.reshape(count_blocks, block_rows, HEADS, HD)
    key_heads = key_rows.reshape(length, HEADS, HD)
    value_heads = value_rows.reshape(length, HEADS, HD)

    @jax.checkpoint
    def one_block(block_item):
        rows_q, first_row = block_item
        scores = jnp.einsum('qhd,khd->hqk', rows_q, key_heads, precision=lax.Precision.HIGHEST) * score_scale
        scores = low_back(scores)
        place_q = first_row + jnp.arange(block_rows, dtype=jnp.int32)
        place_k = jnp.arange(length, dtype=jnp.int32)
        allowed = place_k[None, :] <= place_q[:, None]
        weights = jax.nn.softmax(jnp.where(allowed[None], scores, -1e+30), axis=-1)
        return jnp.einsum('hqk,khd->qhd', low(weights), value_heads, precision=lax.Precision.HIGHEST)
    starts = jnp.arange(count_blocks, dtype=jnp.int32) * block_rows
    result = lax.map(one_block, (query_blocks, starts))
    return result.reshape(length, HEADS * HD)

def forward(seq_rows, w_q, w_k, w_v, w_o, w_u, w_d, gains, biases):
    ln_in = low(layer_norm(seq_rows, gains[0], biases[0]))
    queries = both_round(product(ln_in, w_q))
    key_rows = both_round(product(ln_in, w_k))
    value_rows = both_round(product(ln_in, w_v))
    attended = both_round(attention(queries, key_rows, value_rows))
    mixed = low_back(product(attended, w_o))
    hidden = seq_rows + layer_norm(mixed, gains[1], biases[1])
    ln_mid = low(layer_norm(hidden, gains[2], biases[2]))
    pre_act = low_back(product(ln_mid, w_u))
    active = low(jax.nn.gelu(pre_act))
    output = low_back(product(active, w_d))
    return hidden + layer_norm(output, gains[3], biases[3])

def reference(tokens, cotangent, w_query, w_key, w_value, w_out, w_up, w_down, norm_gain, norm_bias):
    params = (w_query.astype(jnp.float32), w_key.astype(jnp.float32), w_value.astype(jnp.float32), w_out.astype(jnp.float32), w_up.astype(jnp.float32), w_down.astype(jnp.float32), norm_gain, norm_bias)
    seq_in = tokens.astype(jnp.float32).reshape(SEQS, SEQ, D)
    seq_cot = cotangent.astype(jnp.float32).reshape(SEQS, SEQ, D)

    def one_sequence(summed, pair_item):
        seq_rows, seq_grad = pair_item
        result, pull_back = jax.vjp(forward, seq_rows, *params)
        pulled = pull_back(seq_grad)
        summed = tuple((acc_term + new_term for acc_term, new_term in zip(summed, pulled[1:])))
        return (summed, (result, pulled[0]))
    zeros = tuple((jnp.zeros(param.shape, jnp.float32) for param in params))
    summed, (results, input_rows) = lax.scan(one_sequence, zeros, (seq_in, seq_cot))
    block_out = results.reshape(TOKENS, D).astype(jnp.bfloat16)
    input_grad = input_rows.reshape(TOKENS, D)
    return (block_out, input_grad, summed[0], summed[1], summed[2], summed[3], summed[4], summed[5], summed[6], summed[7])
```

```python
import math

import jax
import jax.numpy as jnp
from jax import lax
from jax.sharding import Mesh, PartitionSpec as P

HD = 64


EPS = 1e-05


def normalize(values, gain, bias):
    average = jnp.mean(values, axis=-1, keepdims=True)
    centred = values - average
    inverse = lax.rsqrt(jnp.mean(centred * centred, axis=-1, keepdims=True) + EPS)
    unit_rows = centred * inverse
    return (unit_rows * gain + bias, unit_rows, inverse)


def normalize_back(gradient, unit_rows, inverse, gain):
    scaled = gradient * gain
    inner_sum = (
        scaled
        - jnp.mean(scaled, axis=-1, keepdims=True)
        - unit_rows * jnp.mean(scaled * unit_rows, axis=-1, keepdims=True)
    )
    return (inner_sum * inverse, jnp.sum(gradient * unit_rows, axis=0), jnp.sum(gradient, axis=0))


def masked_scores(rows_q, key_heads, first_row, score_scale):
    scores = (
        jnp.einsum("qgd,kgd->gqk", rows_q, key_heads, preferred_element_type=jnp.float32)
        * score_scale
    )
    place_q = first_row + jnp.arange(rows_q.shape[0], dtype=jnp.int32)
    place_k = jnp.arange(key_heads.shape[0], dtype=jnp.int32)
    allowed = place_k[None, :] <= place_q[:, None]
    return jnp.where(allowed[None], scores, -1e30)


def attend(queries, key_rows, value_rows, block_rows):
    length, width = queries.shape
    groups = width // HD
    score_scale = 1.0 / math.sqrt(HD)
    query_heads = queries.reshape(length, groups, HD)
    key_heads = key_rows.reshape(length, groups, HD)
    value_heads = value_rows.reshape(length, groups, HD)
    out_blocks = []
    totals = []
    for position in range(length // block_rows):
        first_row = position * block_rows
        last_row = first_row + block_rows
        scores = masked_scores(
            query_heads[first_row:last_row], key_heads[:last_row], first_row, score_scale
        )
        row_max = jnp.max(scores, axis=-1, keepdims=True)
        exp_scores = jnp.exp(scores - row_max)
        row_total = jnp.sum(exp_scores, axis=-1, keepdims=True)
        weights = (exp_scores / row_total).astype(jnp.bfloat16)
        out_blocks.append(
            jnp.einsum(
                "gqk,kgd->qgd", weights, value_heads[:last_row], preferred_element_type=jnp.float32
            )
        )
        totals.append(row_max + jnp.log(row_total))
    return (jnp.concatenate(out_blocks, axis=0).reshape(length, width), totals)


def attend_back(queries, key_rows, value_rows, grad_rows, totals, block_rows):
    length, width = queries.shape
    groups = width // HD
    score_scale = 1.0 / math.sqrt(HD)
    query_heads = queries.reshape(length, groups, HD)
    key_heads = key_rows.reshape(length, groups, HD)
    value_heads = value_rows.reshape(length, groups, HD)
    grad_heads = grad_rows.reshape(length, groups, HD)
    grad_keys = jnp.zeros((length, groups, HD), jnp.float32)
    grad_values = jnp.zeros((length, groups, HD), jnp.float32)
    query_parts = []
    for position in range(length // block_rows):
        first_row = position * block_rows
        last_row = first_row + block_rows
        rows_q = query_heads[first_row:last_row]
        scores = masked_scores(rows_q, key_heads[:last_row], first_row, score_scale)
        weights = jnp.exp(scores - totals[position])
        rounded = weights.astype(jnp.bfloat16)
        grad_block = grad_heads[first_row:last_row]
        grad_values = grad_values.at[:last_row].add(
            jnp.einsum("gqk,qgd->kgd", rounded, grad_block, preferred_element_type=jnp.float32)
        )
        grad_weights = jnp.einsum(
            "qgd,kgd->gqk", grad_block, value_heads[:last_row], preferred_element_type=jnp.float32
        )
        inner_sum = jnp.sum(weights * grad_weights, axis=-1, keepdims=True)
        grad_scores = (weights * (grad_weights - inner_sum)).astype(jnp.bfloat16)
        query_parts.append(
            jnp.einsum(
                "gqk,kgd->qgd",
                grad_scores,
                key_heads[:last_row],
                preferred_element_type=jnp.float32,
            )
            * score_scale
        )
        grad_keys = grad_keys.at[:last_row].add(
            jnp.einsum("gqk,qgd->kgd", grad_scores, rows_q, preferred_element_type=jnp.float32)
            * score_scale
        )
    grad_queries = jnp.concatenate(query_parts, axis=0).reshape(length, width).astype(jnp.bfloat16)
    return (
        grad_queries,
        grad_keys.reshape(length, width).astype(jnp.bfloat16),
        grad_values.reshape(length, width).astype(jnp.bfloat16),
    )


def contract_rows(left_op, right_op):
    return lax.dot_general(
        left_op, right_op, (((0,), (0,)), ((), ())), preferred_element_type=jnp.float32
    )


def contract_cols(left_op, right_op):
    return lax.dot_general(
        left_op, right_op, (((1,), (1,)), ((), ())), preferred_element_type=jnp.float32
    )

WIDE = ("outer", "pair")
ALL = ("outer", "pair", "head")


def swap(values):
    return lax.ppermute(values, "pair", [(0, 1), (1, 0)])


def halves(block, axis):
    size = block.shape[axis] // 2
    place = lax.axis_index("pair")
    own = lax.dynamic_slice_in_dim(block, place * size, size, axis)
    other = lax.dynamic_slice_in_dim(block, (1 - place) * size, size, axis)
    return own, other


def in_order(own, other, axis):
    place = lax.axis_index("pair")
    return jnp.where(
        place == 0,
        jnp.concatenate([own, other], axis=axis),
        jnp.concatenate([other, own], axis=axis),
    )


def gather_half(block):
    own, other = halves(block, 1)
    pair_rows = in_order(own, swap(other), 0)
    columns = lax.all_gather(pair_rows, "head", axis=0, tiled=False)
    columns = columns.transpose(1, 0, 2).reshape(pair_rows.shape[0], -1)
    return lax.all_gather(columns, "outer", axis=0, tiled=True)


def scatter_half(grad, groups):
    rows = lax.psum_scatter(grad, "outer", scatter_dimension=0, tiled=True)
    blocks = rows.reshape(rows.shape[0], groups, -1).transpose(1, 0, 2)
    block = lax.psum_scatter(blocks, "head", scatter_dimension=0, tiled=False)
    own, other = halves(block, 0)
    return in_order(own, swap(other), 1)


def on_device(
    tokens, cotangent, w_query, w_key, w_value, w_out, w_up, w_down, norm_gain, norm_bias
):
    groups = lax.axis_size("head")
    rows = tokens.shape[0]
    width = w_query.shape[1]
    bf16 = jnp.bfloat16
    w_attn = lax.all_gather(
        jnp.concatenate([w_query, w_key, w_value], axis=1), WIDE, axis=0, tiled=True
    )
    residual = tokens.astype(jnp.float32)
    norm_a, unit_a, inv_a = normalize(residual, norm_gain[0], norm_bias[0])
    seq_a = lax.all_gather(norm_a.astype(bf16), "head", axis=0, tiled=True)
    full_o = lax.all_gather(
        lax.all_gather(w_out, "head", axis=0, tiled=True).T, WIDE, axis=0, tiled=True
    )
    full_up = gather_half(w_up)
    full_down = gather_half(w_down.T)
    block_rows = min(512, seq_a.shape[0])
    qkv = jnp.dot(seq_a, w_attn, preferred_element_type=jnp.float32).astype(bf16)
    queries, key_rows, value_rows = (qkv[:, i * width : (i + 1) * width] for i in range(3))
    attended, totals = attend(queries, key_rows, value_rows, block_rows)
    attended = lax.all_to_all(
        attended.astype(bf16).reshape(groups, rows, width), "head", 0, 0, tiled=False
    )
    attended = attended.transpose(1, 0, 2).reshape(rows, groups * width)
    mixed = contract_cols(attended, full_o)
    norm_z, unit_z, inv_z = normalize(mixed, norm_gain[1], norm_bias[1])
    hidden = residual + norm_z
    norm_c, unit_c, inv_c = normalize(hidden, norm_gain[2], norm_bias[2])
    rows_c = norm_c.astype(bf16)
    pair_c = jnp.concatenate([rows_c, swap(rows_c)], axis=0)
    pre_act = jnp.dot(pair_c, full_up, preferred_element_type=jnp.float32)
    active, gelu_back = jax.vjp(jax.nn.gelu, pre_act)
    active = active.astype(bf16)
    both = contract_cols(active, full_down)
    output = both[:rows] + swap(both[rows:].astype(bf16)).astype(jnp.float32)
    norm_m, unit_m, inv_m = normalize(output, norm_gain[3], norm_bias[3])
    block_out = (hidden + norm_m).astype(bf16)
    grad_y = cotangent.astype(jnp.float32)
    grad_m, gain_m, bias_m = normalize_back(grad_y, unit_m, inv_m, norm_gain[3])
    rows_gm = grad_m.astype(bf16)
    pair_gm = jnp.concatenate([rows_gm, swap(rows_gm)], axis=0)
    grad_act = jnp.dot(pair_gm, full_down, preferred_element_type=jnp.float32)
    grad_pre = gelu_back(grad_act)[0].astype(bf16)
    both_c = contract_cols(grad_pre, full_up)
    grad_c = both_c[:rows] + swap(both_c[rows:].astype(bf16)).astype(jnp.float32)
    grad_down = scatter_half(contract_rows(pair_gm, active).astype(bf16), groups).T
    grad_up = scatter_half(contract_rows(pair_c, grad_pre).astype(bf16), groups)
    grad_more, gain_c, bias_c = normalize_back(grad_c, unit_c, inv_c, norm_gain[2])
    grad_h = grad_y + grad_more
    grad_z, gain_z, bias_z = normalize_back(grad_h, unit_z, inv_z, norm_gain[1])
    rows_gz = grad_z.astype(bf16)
    grad_att = jnp.dot(rows_gz, full_o, preferred_element_type=jnp.float32).astype(bf16)
    grad_att = grad_att.reshape(rows, groups, width).transpose(1, 0, 2)
    grad_att = lax.all_to_all(grad_att, "head", 0, 0, tiled=False)
    grad_att = grad_att.reshape(groups * rows, width)
    grad_o = contract_rows(rows_gz, attended).astype(bf16)
    grad_o = lax.psum_scatter(grad_o, WIDE, scatter_dimension=0, tiled=True)
    grad_o = grad_o.T.reshape(groups, width, -1)
    grad_o = lax.psum_scatter(grad_o, "head", scatter_dimension=0, tiled=False)
    grad_queries, grad_keys, grad_values = attend_back(
        queries, key_rows, value_rows, grad_att, totals, block_rows
    )
    grad_qkv = jnp.concatenate([grad_queries, grad_keys, grad_values], axis=1)
    grad_a = contract_cols(grad_qkv, w_attn).astype(bf16)
    grad_a = lax.psum_scatter(grad_a, "head", scatter_dimension=0, tiled=True).astype(jnp.float32)
    grad_w = contract_rows(seq_a, grad_qkv).astype(bf16)
    grad_w = lax.psum_scatter(grad_w, WIDE, scatter_dimension=0, tiled=True).astype(jnp.float32)
    grad_first, gain_a, bias_a = normalize_back(grad_a, unit_a, inv_a, norm_gain[0])
    input_grad = grad_h + grad_first
    gain_grad, bias_grad = lax.psum(
        (jnp.stack([gain_a, gain_z, gain_c, gain_m]), jnp.stack([bias_a, bias_z, bias_c, bias_m])),
        ALL,
    )
    return (
        block_out,
        input_grad,
        grad_w[:, :width],
        grad_w[:, width : 2 * width],
        grad_w[:, 2 * width :],
        grad_o.astype(jnp.float32),
        grad_up.astype(jnp.float32),
        grad_down.astype(jnp.float32),
        gain_grad,
        bias_grad,
    )


def solution(mesh):
    wide, head = mesh.shape["wide"], mesh.shape["head"]
    paired = Mesh(mesh.devices.reshape(wide // 2, 2, head), ALL)
    rows = P(ALL, None)
    by_rows = P(WIDE, "head")
    by_cols = P("head", WIDE)
    in_specs = (rows, rows, by_rows, by_rows, by_rows, by_cols, by_rows, by_cols, P(), P())
    out_specs = (rows, rows, by_rows, by_rows, by_rows, by_cols, by_rows, by_cols, P(), P())
    return jax.shard_map(
        on_device, mesh=paired, in_specs=in_specs, out_specs=out_specs, check_vma=False
    )
```

```python
import math

import jax
import jax.numpy as jnp
from jax import lax
from jax.sharding import Mesh, PartitionSpec as P

HD = 64


EPS = 1e-05


def normalize(values, gain, bias):
    average = jnp.mean(values, axis=-1, keepdims=True)
    centred = values - average
    inverse = lax.rsqrt(jnp.mean(centred * centred, axis=-1, keepdims=True) + EPS)
    unit_rows = centred * inverse
    return (unit_rows * gain + bias, unit_rows, inverse)


def normalize_back(gradient, unit_rows, inverse, gain):
    scaled = gradient * gain
    inner_sum = (
        scaled
        - jnp.mean(scaled, axis=-1, keepdims=True)
        - unit_rows * jnp.mean(scaled * unit_rows, axis=-1, keepdims=True)
    )
    return (inner_sum * inverse, jnp.sum(gradient * unit_rows, axis=0), jnp.sum(gradient, axis=0))


def masked_scores(rows_q, key_heads, first_row, score_scale):
    scores = (
        jnp.einsum("qgd,kgd->gqk", rows_q, key_heads, preferred_element_type=jnp.float32)
        * score_scale
    )
    place_q = first_row + jnp.arange(rows_q.shape[0], dtype=jnp.int32)
    place_k = jnp.arange(key_heads.shape[0], dtype=jnp.int32)
    allowed = place_k[None, :] <= place_q[:, None]
    return jnp.where(allowed[None], scores, -1e30)


def attend(queries, key_rows, value_rows, block_rows):
    length, width = queries.shape
    groups = width // HD
    score_scale = 1.0 / math.sqrt(HD)
    query_heads = queries.reshape(length, groups, HD)
    key_heads = key_rows.reshape(length, groups, HD)
    value_heads = value_rows.reshape(length, groups, HD)
    out_blocks = []
    totals = []
    for position in range(length // block_rows):
        first_row = position * block_rows
        last_row = first_row + block_rows
        scores = masked_scores(
            query_heads[first_row:last_row], key_heads[:last_row], first_row, score_scale
        )
        row_max = jnp.max(scores, axis=-1, keepdims=True)
        exp_scores = jnp.exp(scores - row_max)
        row_total = jnp.sum(exp_scores, axis=-1, keepdims=True)
        weights = (exp_scores / row_total).astype(jnp.bfloat16)
        out_blocks.append(
            jnp.einsum(
                "gqk,kgd->qgd", weights, value_heads[:last_row], preferred_element_type=jnp.float32
            )
        )
        totals.append(row_max + jnp.log(row_total))
    return (jnp.concatenate(out_blocks, axis=0).reshape(length, width), totals)


def attend_back(queries, key_rows, value_rows, grad_rows, totals, block_rows):
    length, width = queries.shape
    groups = width // HD
    score_scale = 1.0 / math.sqrt(HD)
    query_heads = queries.reshape(length, groups, HD)
    key_heads = key_rows.reshape(length, groups, HD)
    value_heads = value_rows.reshape(length, groups, HD)
    grad_heads = grad_rows.reshape(length, groups, HD)
    grad_keys = jnp.zeros((length, groups, HD), jnp.float32)
    grad_values = jnp.zeros((length, groups, HD), jnp.float32)
    query_parts = []
    for position in range(length // block_rows):
        first_row = position * block_rows
        last_row = first_row + block_rows
        rows_q = query_heads[first_row:last_row]
        scores = masked_scores(rows_q, key_heads[:last_row], first_row, score_scale)
        weights = jnp.exp(scores - totals[position])
        rounded = weights.astype(jnp.bfloat16)
        grad_block = grad_heads[first_row:last_row]
        grad_values = grad_values.at[:last_row].add(
            jnp.einsum("gqk,qgd->kgd", rounded, grad_block, preferred_element_type=jnp.float32)
        )
        grad_weights = jnp.einsum(
            "qgd,kgd->gqk", grad_block, value_heads[:last_row], preferred_element_type=jnp.float32
        )
        inner_sum = jnp.sum(weights * grad_weights, axis=-1, keepdims=True)
        grad_scores = (weights * (grad_weights - inner_sum)).astype(jnp.bfloat16)
        query_parts.append(
            jnp.einsum(
                "gqk,kgd->qgd",
                grad_scores,
                key_heads[:last_row],
                preferred_element_type=jnp.float32,
            )
            * score_scale
        )
        grad_keys = grad_keys.at[:last_row].add(
            jnp.einsum("gqk,qgd->kgd", grad_scores, rows_q, preferred_element_type=jnp.float32)
            * score_scale
        )
    grad_queries = jnp.concatenate(query_parts, axis=0).reshape(length, width).astype(jnp.bfloat16)
    return (
        grad_queries,
        grad_keys.reshape(length, width).astype(jnp.bfloat16),
        grad_values.reshape(length, width).astype(jnp.bfloat16),
    )


def contract_rows(left_op, right_op):
    return lax.dot_general(
        left_op, right_op, (((0,), (0,)), ((), ())), preferred_element_type=jnp.float32
    )


def contract_cols(left_op, right_op):
    return lax.dot_general(
        left_op, right_op, (((1,), (1,)), ((), ())), preferred_element_type=jnp.float32
    )


WIDE = ("outer", "pair")
ALL = ("outer", "pair", "head")
LINE = ("pair", "head")
HEADS = 4


def swap(values):
    return lax.ppermute(values, "pair", [(0, 1), (1, 0)])


def send(values, moves):
    return lax.ppermute(values, LINE, [(a * HEADS + b, c * HEADS + d) for (a, b), (c, d) in moves])


def both(moves):
    return [((p, a), (p, b)) for p in range(2) for a, b in moves]


def shift(values, step):
    return lax.ppermute(values, "head", [(i, (i + step) % HEADS) for i in range(HEADS)])


def halves(block, axis):
    size = block.shape[axis] // 2
    place = lax.axis_index("pair")
    own = lax.dynamic_slice_in_dim(block, place * size, size, axis)
    other = lax.dynamic_slice_in_dim(block, (1 - place) * size, size, axis)
    return own, other


def in_order(own, other, axis):
    place = lax.axis_index("pair")
    return jnp.where(
        place == 0,
        jnp.concatenate([own, other], axis=axis),
        jnp.concatenate([other, own], axis=axis),
    )


def after(values, earlier):
    return lax.optimization_barrier((values, earlier))[0]


def spread(block, axis):
    return jnp.concatenate([block] + [shift(block, k) for k in range(1, HEADS)], axis=axis)


def collect(blocks):
    total = blocks[0].astype(jnp.float32)
    for k in range(1, HEADS):
        total = total + shift(blocks[k], -k).astype(jnp.float32)
    return total


def half_rows(block):
    own, other = halves(block, 1)
    return in_order(own, swap(other), 0)


def scatter_half(grad):
    rows = lax.psum_scatter(grad, "outer", scatter_dimension=0, tiled=True)
    block = collect(jnp.split(rows, HEADS, axis=1)).astype(jnp.bfloat16)
    own, other = halves(block, 0)
    return in_order(own, swap(other), 1).astype(jnp.float32)


FORWARD = [((z // 2, z), (1 - z // 2, z)) for z in range(HEADS)]


def sequence_rows(block):
    place = lax.axis_index("head")
    holds = lax.axis_index("pair") == place // 2
    inner = (place == 1) | (place == 2)
    near = send(
        block,
        [((0, 0), (0, 1)), ((0, 1), (0, 0)), ((1, 2), (1, 3)), ((1, 3), (1, 2))],
    )
    next_in = send(block, [((0, 2), (0, 1)), ((1, 1), (1, 2))])
    last_in = send(block, [((0, 3), (0, 1)), ((1, 0), (1, 2))])
    outward = [((0, 1), (0, 0)), ((1, 2), (1, 3))]
    next_out = send(next_in, outward)
    last_out = send(last_in, outward)
    pieces = (
        block,
        near,
        jnp.where(inner, next_in, next_out),
        jnp.where(inner, last_in, last_out),
    )
    own, near, following, last = (jnp.where(holds, v, send(v, FORWARD)) for v in pieces)
    first = jnp.where(place % 2 == 0, own, near)
    second = jnp.where(place % 2 == 0, near, own)
    low = place < 2
    return jnp.concatenate(
        [
            jnp.where(low, first, last),
            jnp.where(low, second, following),
            jnp.where(low, following, first),
            jnp.where(low, last, second),
        ],
        axis=0,
    )


def sequence_sum(partial):
    place = lax.axis_index("head")
    pair = lax.axis_index("pair")
    low = place < 2
    inner = (place == 1) | (place == 2)
    own, other = halves(partial, 1)
    half = own.astype(jnp.float32) + swap(other).astype(jnp.float32)
    rows = half.shape[0] // HEADS

    def block(i):
        index = jnp.where(low, i, HEADS - 1 - i)
        return lax.dynamic_slice_in_dim(half, index * rows, rows, 0)

    inward = both([(0, 1), (3, 2)])
    near_moves = both([(0, 1), (1, 0), (2, 3), (3, 2)])
    bf16 = jnp.bfloat16
    last = block(3) + send(block(3).astype(bf16), inward).astype(jnp.float32)
    last = send(last.astype(bf16), both([(1, 3), (2, 0)]))
    following = block(2) + send(block(2).astype(bf16), inward).astype(jnp.float32)
    following = send(following.astype(bf16), both([(1, 2), (2, 1)]))
    away = jnp.where(inner, block(0), block(1)).astype(bf16)
    mine = jnp.where(inner, block(1), block(0)) + send(away, near_moves).astype(jnp.float32)
    far = jnp.where(inner, following, last).astype(jnp.float32)
    keeps = pair == place // 2
    kept = jnp.where(keeps, mine, far)
    given = swap(jnp.where(keeps, far, mine).astype(bf16)).astype(jnp.float32)
    return in_order(kept, given, 1)


def group_moves(k):
    moves = []
    for p in range(2):
        for z in range(HEADS):
            group = 2 * (z % 2) + p
            moves.append(((p, z), (z // 2, (group + k) % HEADS)))
    return moves


def column_moves(k):
    moves = []
    for p in range(2):
        for group in range(HEADS):
            moves.append(((p, group), (group % 2, group // 2 + 2 * (p ^ k))))
    return moves


def turned(moves):
    return [(b, a) for a, b in moves]


def group_to_rows(values):
    rows = values.shape[0] // HEADS
    group = 2 * (lax.axis_index("head") % 2) + lax.axis_index("pair")
    parts = []
    for k in range(HEADS):
        start = (group + k) % HEADS * rows
        parts.append(send(lax.dynamic_slice_in_dim(values, start, rows, 0), group_moves(k)))
    return jnp.concatenate(parts, axis=1)


def rows_to_group(values):
    group = 2 * (lax.axis_index("head") % 2) + lax.axis_index("pair")
    rows = values.shape[0]
    parts = [
        send(part, turned(group_moves(k)))
        for k, part in enumerate(jnp.split(values, HEADS, axis=1))
    ]
    twice = jnp.concatenate(parts + parts, axis=0)
    start = (HEADS - group) % HEADS * rows
    return lax.dynamic_slice_in_dim(twice, start, HEADS * rows, 0)


def sum_all(values):
    for axis in ALL:
        size = lax.axis_size(axis)
        step = 1
        while step < size:
            values = values + lax.ppermute(values, axis, [(i, i ^ step) for i in range(size)])
            step *= 2
    return values


def on_device(
    tokens, cotangent, w_query, w_key, w_value, w_out, w_up, w_down, norm_gain, norm_bias
):
    rows = tokens.shape[0]
    width = w_query.shape[1]
    model = w_query.shape[0] * lax.axis_size("outer") * 2
    bf16 = jnp.bfloat16
    f32 = jnp.float32
    late = lax.axis_index("head") // 2
    residual = tokens.astype(f32)
    norm_a, unit_a, inv_a = normalize(residual, norm_gain[0], norm_bias[0])

    w_cols = jnp.concatenate([w_query, w_key, w_value], axis=1)
    w_first, w_second = (send(w_cols, column_moves(k)) for k in range(2))
    w_cols = jnp.where(
        late == 0,
        jnp.concatenate([w_first, w_second], axis=0),
        jnp.concatenate([w_second, w_first], axis=0),
    )
    w_cols = lax.all_gather(w_cols, "outer", axis=0, tiled=True)
    seq_a = sequence_rows(norm_a.astype(bf16))
    out_rows = spread(w_out.T, 1)
    out_own = lax.all_gather(out_rows, "outer", axis=0, tiled=False)
    full_up = lax.all_gather(spread(half_rows(w_up), 1), "outer", axis=0, tiled=True)
    full_down = lax.all_gather(spread(half_rows(w_down.T), 1), "outer", axis=0, tiled=True)

    block_rows = min(512, seq_a.shape[0])
    qkv = jnp.dot(seq_a, w_cols, preferred_element_type=f32).astype(bf16)
    queries, key_rows, value_rows = (qkv[:, i * width : (i + 1) * width] for i in range(3))
    attended, totals = attend(queries, key_rows, value_rows, block_rows)
    attended = group_to_rows(attended.astype(bf16))
    out_other = swap(out_own)
    place = lax.axis_index("pair")
    full_o = jnp.stack(
        [jnp.where(place == 0, out_own, out_other), jnp.where(place == 0, out_other, out_own)],
        axis=1,
    ).reshape(model, -1)
    mixed = contract_cols(attended, full_o)
    norm_z, unit_z, inv_z = normalize(mixed, norm_gain[1], norm_bias[1])
    hidden = residual + norm_z
    norm_c, unit_c, inv_c = normalize(hidden, norm_gain[2], norm_bias[2])
    rows_c = norm_c.astype(bf16)
    pair_c = jnp.concatenate([rows_c, swap(rows_c)], axis=0)
    pre_act = jnp.dot(pair_c, full_up, preferred_element_type=f32)
    active, gelu_back = jax.vjp(jax.nn.gelu, pre_act)
    active = active.astype(bf16)
    both_m = contract_cols(active, full_down)
    output = both_m[:rows] + swap(both_m[rows:].astype(bf16)).astype(f32)
    norm_m, unit_m, inv_m = normalize(output, norm_gain[3], norm_bias[3])
    block_out = (hidden + norm_m).astype(bf16)

    grad_y = cotangent.astype(f32)
    grad_m, gain_m, bias_m = normalize_back(grad_y, unit_m, inv_m, norm_gain[3])
    rows_gm = grad_m.astype(bf16)
    pair_gm = jnp.concatenate([rows_gm, swap(rows_gm)], axis=0)
    grad_act = jnp.dot(pair_gm, full_down, preferred_element_type=f32)
    grad_pre = gelu_back(grad_act)[0].astype(bf16)
    both_c = contract_cols(grad_pre, full_up)
    grad_c = both_c[:rows] + swap(both_c[rows:].astype(bf16)).astype(f32)
    grad_down = scatter_half(contract_rows(pair_gm, active).astype(bf16)).T
    grad_up = scatter_half(contract_rows(pair_c, grad_pre).astype(bf16))
    grad_more, gain_c, bias_c = normalize_back(grad_c, unit_c, inv_c, norm_gain[2])
    grad_h = grad_y + grad_more
    grad_z, gain_z, bias_z = normalize_back(grad_h, unit_z, inv_z, norm_gain[1])
    rows_gz = grad_z.astype(bf16)
    grad_att = jnp.dot(rows_gz, full_o, preferred_element_type=f32).astype(bf16)
    grad_att = rows_to_group(grad_att)
    grad_o = contract_rows(rows_gz, attended).astype(bf16)
    grad_o = grad_o.reshape(-1, 2, w_out.shape[1], attended.shape[1])
    own_o, other_o = halves(grad_o, 1)
    grad_o = (own_o.astype(f32) + swap(other_o).astype(f32)).astype(bf16)
    grad_o = grad_o.reshape(-1, attended.shape[1])
    grad_o = lax.psum_scatter(grad_o, "outer", scatter_dimension=0, tiled=True)
    grad_o = collect(jnp.split(grad_o, HEADS, axis=1)).T
    grad_queries, grad_keys, grad_values = attend_back(
        queries, key_rows, value_rows, grad_att, totals, block_rows
    )
    grad_qkv = jnp.concatenate([grad_queries, grad_keys, grad_values], axis=1)
    grad_a = sequence_sum(contract_cols(grad_qkv, w_cols).astype(bf16))
    grad_w = contract_rows(seq_a, grad_qkv).astype(bf16)
    grad_w = lax.psum_scatter(grad_w, "outer", scatter_dimension=0, tiled=True)
    size = grad_w.shape[0] // 2
    parts = [
        send(
            lax.dynamic_slice_in_dim(grad_w, jnp.where(late == k, 0, size), size, 0),
            turned(column_moves(k)),
        ).astype(f32)
        for k in range(2)
    ]
    grad_w = parts[0] + parts[1]
    grad_first, gain_a, bias_a = normalize_back(grad_a, unit_a, inv_a, norm_gain[0])
    input_grad = grad_h + grad_first
    sums = sum_all(jnp.stack([gain_a, gain_z, gain_c, gain_m, bias_a, bias_z, bias_c, bias_m]))
    return (
        block_out,
        input_grad,
        grad_w[:, :width],
        grad_w[:, width : 2 * width],
        grad_w[:, 2 * width :],
        grad_o,
        grad_up,
        grad_down,
        sums[:4],
        sums[4:],
    )


def solution(mesh):
    wide, head = mesh.shape["wide"], mesh.shape["head"]
    assert head == HEADS and wide % 2 == 0
    paired = Mesh(mesh.devices.reshape(wide // 2, 2, head), ALL)
    rows = P(ALL, None)
    by_rows = P(WIDE, "head")
    by_cols = P("head", WIDE)
    in_specs = (rows, rows, by_rows, by_rows, by_rows, by_cols, by_rows, by_cols, P(), P())
    out_specs = (rows, rows, by_rows, by_rows, by_rows, by_cols, by_rows, by_cols, P(), P())
    return jax.shard_map(
        on_device, mesh=paired, in_specs=in_specs, out_specs=out_specs, check_vma=False
    )
```

```python
import math

import jax
import jax.numpy as jnp
from jax import lax
from jax.sharding import Mesh, PartitionSpec as P


HD = 64


EPS = 1e-05


def normalize(values, gain, bias):
    average = jnp.mean(values, axis=-1, keepdims=True)
    centred = values - average
    inverse = lax.rsqrt(jnp.mean(centred * centred, axis=-1, keepdims=True) + EPS)
    unit_rows = centred * inverse
    return (unit_rows * gain + bias, unit_rows, inverse)


def normalize_back(gradient, unit_rows, inverse, gain):
    scaled = gradient * gain
    inner_sum = (
        scaled
        - jnp.mean(scaled, axis=-1, keepdims=True)
        - unit_rows * jnp.mean(scaled * unit_rows, axis=-1, keepdims=True)
    )
    return (inner_sum * inverse, jnp.sum(gradient * unit_rows, axis=0), jnp.sum(gradient, axis=0))


def masked_scores(rows_q, key_heads, first_row, score_scale):
    scores = (
        jnp.einsum("qgd,kgd->gqk", rows_q, key_heads, preferred_element_type=jnp.float32)
        * score_scale
    )
    place_q = first_row + jnp.arange(rows_q.shape[0], dtype=jnp.int32)
    place_k = jnp.arange(key_heads.shape[0], dtype=jnp.int32)
    allowed = place_k[None, :] <= place_q[:, None]
    return jnp.where(allowed[None], scores, -1e30)


def attend(queries, key_rows, value_rows, block_rows):
    length, width = queries.shape
    groups = width // HD
    score_scale = 1.0 / math.sqrt(HD)
    query_heads = queries.reshape(length, groups, HD)
    key_heads = key_rows.reshape(length, groups, HD)
    value_heads = value_rows.reshape(length, groups, HD)
    out_blocks = []
    totals = []
    for position in range(length // block_rows):
        first_row = position * block_rows
        last_row = first_row + block_rows
        scores = masked_scores(
            query_heads[first_row:last_row], key_heads[:last_row], first_row, score_scale
        )
        row_max = jnp.max(scores, axis=-1, keepdims=True)
        exp_scores = jnp.exp(scores - row_max)
        row_total = jnp.sum(exp_scores, axis=-1, keepdims=True)
        weights = (exp_scores / row_total).astype(jnp.bfloat16)
        out_blocks.append(
            jnp.einsum(
                "gqk,kgd->qgd", weights, value_heads[:last_row], preferred_element_type=jnp.float32
            )
        )
        totals.append(row_max + jnp.log(row_total))
    return (jnp.concatenate(out_blocks, axis=0).reshape(length, width), totals)


def attend_back(queries, key_rows, value_rows, grad_rows, totals, block_rows, first):
    length, width = queries.shape
    groups = width // HD
    score_scale = 1.0 / math.sqrt(HD)
    query_heads = queries.reshape(length, groups, HD)
    key_heads = key_rows.reshape(length, groups, HD)
    value_heads = value_rows.reshape(length, groups, HD)
    grad_heads = grad_rows.reshape(length, groups, HD)
    grad_keys = jnp.zeros((length, groups, HD), jnp.float32)
    grad_values = jnp.zeros((length, groups, HD), jnp.float32)
    query_parts = []
    for position in range(length // block_rows):
        first_row = position * block_rows
        last_row = first_row + block_rows
        rows_q = query_heads[first_row:last_row]
        if last_row == length:
            rows_q, grad_rows = lax.optimization_barrier(((rows_q, grad_heads), first))[0]
            grad_heads = grad_rows
        scores = masked_scores(rows_q, key_heads[:last_row], first_row, score_scale)
        weights = jnp.exp(scores - totals[position])
        rounded = weights.astype(jnp.bfloat16)
        grad_block = grad_heads[first_row:last_row]
        grad_values = grad_values.at[:last_row].add(
            jnp.einsum("gqk,qgd->kgd", rounded, grad_block, preferred_element_type=jnp.float32)
        )
        grad_weights = jnp.einsum(
            "qgd,kgd->gqk", grad_block, value_heads[:last_row], preferred_element_type=jnp.float32
        )
        inner_sum = jnp.sum(weights * grad_weights, axis=-1, keepdims=True)
        grad_scores = (weights * (grad_weights - inner_sum)).astype(jnp.bfloat16)
        query_parts.append(
            jnp.einsum(
                "gqk,kgd->qgd",
                grad_scores,
                key_heads[:last_row],
                preferred_element_type=jnp.float32,
            )
            * score_scale
        )
        grad_keys = grad_keys.at[:last_row].add(
            jnp.einsum("gqk,qgd->kgd", grad_scores, rows_q, preferred_element_type=jnp.float32)
            * score_scale
        )
    grad_queries = jnp.concatenate(query_parts, axis=0).reshape(length, width).astype(jnp.bfloat16)
    return (
        grad_queries,
        grad_keys.reshape(length, width).astype(jnp.bfloat16),
        grad_values.reshape(length, width).astype(jnp.bfloat16),
    )


def contract_rows(left_op, right_op):
    return lax.dot_general(
        left_op, right_op, (((0,), (0,)), ((), ())), preferred_element_type=jnp.float32
    )


def contract_cols(left_op, right_op):
    return lax.dot_general(
        left_op, right_op, (((1,), (1,)), ((), ())), preferred_element_type=jnp.float32
    )


WIDE = ("outer", "pair")
ALL = ("outer", "pair", "head")
LINE = ("pair", "head")
HEADS = 4


def swap(values):
    return lax.ppermute(values, "pair", [(0, 1), (1, 0)])


def send(values, moves):
    return lax.ppermute(values, LINE, [(a * HEADS + b, c * HEADS + d) for (a, b), (c, d) in moves])


def both(moves):
    return [((p, a), (p, b)) for p in range(2) for a, b in moves]


def shift(values, step):
    return lax.ppermute(values, "head", [(i, (i + step) % HEADS) for i in range(HEADS)])


def halves(block, axis):
    size = block.shape[axis] // 2
    place = lax.axis_index("pair")
    own = lax.dynamic_slice_in_dim(block, place * size, size, axis)
    other = lax.dynamic_slice_in_dim(block, (1 - place) * size, size, axis)
    return own, other


def in_order(own, other, axis):
    place = lax.axis_index("pair")
    return jnp.where(
        place == 0,
        jnp.concatenate([own, other], axis=axis),
        jnp.concatenate([other, own], axis=axis),
    )


def after(values, earlier):
    return lax.optimization_barrier((values, earlier))[0]


def spread(block):
    return [block] + [shift(block, k) for k in range(1, HEADS)]


def collect(blocks):
    total = blocks[0].astype(jnp.float32)
    for k in range(1, HEADS):
        total = total + shift(blocks[k], -k).astype(jnp.float32)
    return total


def half_rows(block):
    own, other = halves(block, 1)
    return in_order(own, swap(other), 0)


def scatter_half(rows):
    block = collect(jnp.split(rows, HEADS, axis=1)).astype(jnp.bfloat16)
    own, other = halves(block, 0)
    return in_order(own, swap(other), 1).astype(jnp.float32)


FORWARD = [((z // 2, z), (1 - z // 2, z)) for z in range(HEADS)]


def sequence_rows(block):
    place = lax.axis_index("head")
    holds = lax.axis_index("pair") == place // 2
    inner = (place == 1) | (place == 2)
    near = send(
        block,
        [((0, 0), (0, 1)), ((0, 1), (0, 0)), ((1, 2), (1, 3)), ((1, 3), (1, 2))],
    )
    next_in = send(block, [((0, 2), (0, 1)), ((1, 1), (1, 2))])
    last_in = send(block, [((0, 3), (0, 1)), ((1, 0), (1, 2))])
    outward = [((0, 1), (0, 0)), ((1, 2), (1, 3))]
    next_out = send(next_in, outward)
    last_out = send(last_in, outward)
    pieces = (
        block,
        near,
        jnp.where(inner, next_in, next_out),
        jnp.where(inner, last_in, last_out),
    )
    own, near, following, last = (jnp.where(holds, v, send(v, FORWARD)) for v in pieces)
    first = jnp.where(place % 2 == 0, own, near)
    second = jnp.where(place % 2 == 0, near, own)
    low = place < 2
    joined = jnp.concatenate(
        [
            jnp.where(low, first, last),
            jnp.where(low, second, following),
            jnp.where(low, following, first),
            jnp.where(low, last, second),
        ],
        axis=0,
    )
    return joined, pieces[1]


def sequence_sum(partial):
    place = lax.axis_index("head")
    pair = lax.axis_index("pair")
    low = place < 2
    inner = (place == 1) | (place == 2)
    rows = partial.shape[0] // HEADS

    def block(i):
        index = jnp.where(low, i, HEADS - 1 - i)
        piece = lax.dynamic_slice_in_dim(partial, index * rows, rows, 0)
        own, other = halves(piece, 1)
        return own.astype(jnp.float32) + swap(other).astype(jnp.float32)

    inward = both([(0, 1), (3, 2)])
    near_moves = both([(0, 1), (1, 0), (2, 3), (3, 2)])
    bf16 = jnp.bfloat16
    fourth, third, second, first = (block(i) for i in reversed(range(HEADS)))
    last = fourth + send(fourth.astype(bf16), inward).astype(jnp.float32)
    last = send(last.astype(bf16), both([(1, 3), (2, 0)]))
    following = third + send(third.astype(bf16), inward).astype(jnp.float32)
    following = send(following.astype(bf16), both([(1, 2), (2, 1)]))
    away = jnp.where(inner, first, second).astype(bf16)
    mine = jnp.where(inner, second, first) + send(away, near_moves).astype(jnp.float32)
    far = jnp.where(inner, following, last).astype(jnp.float32)
    keeps = pair == place // 2
    arrived = mine
    kept = jnp.where(keeps, mine, far)
    given = swap(jnp.where(keeps, far, mine).astype(bf16)).astype(jnp.float32)
    return in_order(kept, given, 1), arrived


def group_moves(k):
    moves = []
    for p in range(2):
        for z in range(HEADS):
            group = 2 * (z % 2) + p
            moves.append(((p, z), (z // 2, (group + k) % HEADS)))
    return moves


def column_moves(k):
    moves = []
    for p in range(2):
        for group in range(HEADS):
            moves.append(((p, group), (group % 2, group // 2 + 2 * (p ^ k))))
    return moves


def turned(moves):
    return [(b, a) for a, b in moves]


def group_to_rows(values):
    rows = values.shape[0] // HEADS
    group = 2 * (lax.axis_index("head") % 2) + lax.axis_index("pair")
    parts = []
    for k in range(HEADS):
        start = (group + k) % HEADS * rows
        parts.append(send(lax.dynamic_slice_in_dim(values, start, rows, 0), group_moves(k)))
    return jnp.concatenate(parts, axis=1)


def rows_to_group(values):
    odd = lax.axis_index("pair") == 1
    upper = lax.axis_index("head") % 2 == 1
    parts = [
        send(part, turned(group_moves(k)))
        for k, part in enumerate(jnp.split(values, HEADS, axis=1))
    ]
    parts = [jnp.where(odd, parts[k - 1], parts[k]) for k in range(HEADS)]
    return jnp.concatenate(
        [jnp.where(upper, parts[k - 2], parts[k]) for k in range(HEADS)], axis=0
    )


def sum_all(values):
    for axis in ALL:
        size = lax.axis_size(axis)
        step = 1
        while step < size:
            values = values + lax.ppermute(values, axis, [(i, i ^ step) for i in range(size)])
            step *= 2
    return values


def on_device(
    tokens, cotangent, w_query, w_key, w_value, w_out, w_up, w_down, norm_gain, norm_bias
):
    rows = tokens.shape[0]
    width = w_query.shape[1]
    model = w_query.shape[0] * lax.axis_size("outer") * 2
    bf16 = jnp.bfloat16
    f32 = jnp.float32
    late = lax.axis_index("head") // 2
    residual = tokens.astype(f32)
    norm_a, unit_a, inv_a = normalize(residual, norm_gain[0], norm_bias[0])

    w_cols = jnp.concatenate([w_query, w_key, w_value], axis=1)
    w_first, w_second = (send(w_cols, column_moves(k)) for k in range(2))
    w_cols = jnp.where(
        late == 0,
        jnp.concatenate([w_first, w_second], axis=0),
        jnp.concatenate([w_second, w_first], axis=0),
    )
    out_parts = spread(w_out.T)
    out_low = jnp.concatenate(out_parts[: HEADS // 2], axis=1)
    out_high = jnp.concatenate(out_parts[HEADS // 2 :], axis=1)
    attention = jnp.concatenate(
        [w_cols, jnp.concatenate([out_low, out_high], axis=0)], axis=1
    )
    attention = lax.all_gather(attention, "outer", axis=0, tiled=True)
    w_cols = attention[:, : 3 * width]
    out_own = attention[:, 3 * width :].reshape(-1, 2, w_out.shape[1], 2 * width)
    out_own = jnp.concatenate([out_own[:, 0], out_own[:, 1]], axis=2)
    seq_a, near = sequence_rows(norm_a.astype(bf16))
    up_parts = spread(after(half_rows(w_up), near))
    full_up = lax.all_gather(jnp.concatenate(up_parts, axis=1), "outer", axis=0, tiled=True)
    down_parts = spread(after(half_rows(w_down.T), up_parts))

    block_rows = min(512, seq_a.shape[0])
    qkv = jnp.dot(seq_a, w_cols, preferred_element_type=f32).astype(bf16)
    down_parts = after(down_parts, qkv)
    full_down = lax.all_gather(jnp.concatenate(down_parts, axis=1), "outer", axis=0, tiled=True)
    queries, key_rows, value_rows = (qkv[:, i * width : (i + 1) * width] for i in range(3))
    attended, totals = attend(queries, key_rows, value_rows, block_rows)
    attended = group_to_rows(attended.astype(bf16))
    out_other = swap(out_own)
    place = lax.axis_index("pair")
    full_o = jnp.stack(
        [jnp.where(place == 0, out_own, out_other), jnp.where(place == 0, out_other, out_own)],
        axis=1,
    ).reshape(model, -1)
    mixed = contract_cols(attended, full_o)
    norm_z, unit_z, inv_z = normalize(mixed, norm_gain[1], norm_bias[1])
    hidden = residual + norm_z
    norm_c, unit_c, inv_c = normalize(hidden, norm_gain[2], norm_bias[2])
    rows_c = norm_c.astype(bf16)
    pair_c = jnp.concatenate([rows_c, swap(rows_c)], axis=0)
    pre_act = jnp.dot(pair_c, full_up, preferred_element_type=f32)
    active, gelu_back = jax.vjp(jax.nn.gelu, pre_act)
    active = active.astype(bf16)
    both_m = contract_cols(active, full_down)
    output = both_m[:rows] + swap(both_m[rows:].astype(bf16)).astype(f32)
    norm_m, unit_m, inv_m = normalize(output, norm_gain[3], norm_bias[3])
    block_out = (hidden + norm_m).astype(bf16)

    grad_y = cotangent.astype(f32)
    grad_m, gain_m, bias_m = normalize_back(grad_y, unit_m, inv_m, norm_gain[3])
    rows_gm = grad_m.astype(bf16)
    pair_gm = jnp.concatenate([rows_gm, swap(rows_gm)], axis=0)
    grad_act = jnp.dot(pair_gm, full_down, preferred_element_type=f32)
    grad_pre = gelu_back(grad_act)[0].astype(bf16)
    both_c = contract_cols(grad_pre, full_up)
    grad_c = both_c[:rows] + swap(both_c[rows:].astype(bf16)).astype(f32)
    grad_down = contract_rows(pair_gm, active).astype(bf16)
    grad_up = contract_rows(pair_c, grad_pre).astype(bf16)
    grad_more, gain_c, bias_c = normalize_back(grad_c, unit_c, inv_c, norm_gain[2])
    grad_h = grad_y + grad_more
    grad_z, gain_z, bias_z = normalize_back(grad_h, unit_z, inv_z, norm_gain[1])
    rows_gz = grad_z.astype(bf16)
    grad_att = jnp.dot(rows_gz, full_o, preferred_element_type=f32).astype(bf16)
    grad_att = rows_to_group(grad_att)
    grad_o = contract_rows(rows_gz, attended).astype(bf16)
    grad_o = grad_o.reshape(-1, 2, w_out.shape[1], attended.shape[1])
    own_o, other_o = halves(grad_o, 1)
    grad_o = (own_o.astype(f32) + swap(other_o).astype(f32)).astype(bf16)
    grad_o = grad_o.reshape(-1, attended.shape[1])
    grad_att = after(grad_att, (grad_down, grad_up, grad_o))
    grad_down = lax.psum_scatter(grad_down, "outer", scatter_dimension=0, tiled=True)
    grad_up = lax.psum_scatter(grad_up, "outer", scatter_dimension=0, tiled=True)
    grad_queries, grad_keys, grad_values = attend_back(
        queries, key_rows, value_rows, grad_att, totals, block_rows, grad_down
    )
    grad_down = scatter_half(grad_down).T
    grad_qkv = jnp.concatenate([grad_queries, grad_keys, grad_values], axis=1)
    grad_qkv = after(grad_qkv, grad_down)
    grad_a = contract_cols(grad_qkv, w_cols).astype(bf16)
    grad_w = contract_rows(seq_a, after(grad_qkv, grad_a)).astype(bf16)
    grad_a, arrived = sequence_sum(grad_a)
    grad_o = grad_o.reshape(-1, 1, w_out.shape[1], attended.shape[1])
    grad_o = jnp.concatenate(jnp.split(grad_o, 2, axis=3), axis=1).reshape(model, -1)
    grad_w = after(jnp.concatenate([grad_w, grad_o], axis=1), grad_up)
    grad_w = lax.psum_scatter(grad_w, "outer", scatter_dimension=0, tiled=True)
    grad_w, grad_o = grad_w[:, : 3 * width], grad_w[:, 3 * width :]
    grad_o = collect(
        [
            grad_o[i * w_out.shape[1] : (i + 1) * w_out.shape[1], j * width : (j + 1) * width]
            for i in range(2)
            for j in range(2)
        ]
    ).T
    size = grad_w.shape[0] // 2
    parts = [
        send(
            lax.dynamic_slice_in_dim(grad_w, jnp.where(late == k, 0, size), size, 0),
            turned(column_moves(k)),
        ).astype(f32)
        for k in range(2)
    ]
    grad_w = parts[0] + parts[1]
    grad_up = scatter_half(after(grad_up, arrived))
    grad_first, gain_a, bias_a = normalize_back(grad_a, unit_a, inv_a, norm_gain[0])
    input_grad = grad_h + grad_first
    sums = sum_all(jnp.stack([gain_a, gain_z, gain_c, gain_m, bias_a, bias_z, bias_c, bias_m]))
    return (
        block_out,
        input_grad,
        grad_w[:, :width],
        grad_w[:, width : 2 * width],
        grad_w[:, 2 * width :],
        grad_o,
        grad_up,
        grad_down,
        sums[:4],
        sums[4:],
    )


def solution(mesh):
    wide, head = mesh.shape["wide"], mesh.shape["head"]
    assert head == HEADS and wide % 2 == 0
    paired = Mesh(mesh.devices.reshape(wide // 2, 2, head), ALL)
    rows = P(ALL, None)
    by_rows = P(WIDE, "head")
    by_cols = P("head", WIDE)
    in_specs = (rows, rows, by_rows, by_rows, by_rows, by_cols, by_rows, by_cols, P(), P())
    out_specs = (rows, rows, by_rows, by_rows, by_rows, by_cols, by_rows, by_cols, P(), P())
    return jax.shard_map(
        on_device, mesh=paired, in_specs=in_specs, out_specs=out_specs, check_vma=False
    )
```

```python
import math

import jax
import jax.numpy as jnp
from jax import lax
from jax.sharding import Mesh, PartitionSpec as P


HD = 64


EPS = 1e-05


def normalize(values, gain, bias):
    average = jnp.mean(values, axis=-1, keepdims=True)
    centred = values - average
    inverse = lax.rsqrt(jnp.mean(centred * centred, axis=-1, keepdims=True) + EPS)
    unit_rows = centred * inverse
    return (unit_rows * gain + bias, unit_rows, inverse)


def normalize_back(gradient, unit_rows, inverse, gain):
    scaled = gradient * gain
    inner_sum = (
        scaled
        - jnp.mean(scaled, axis=-1, keepdims=True)
        - unit_rows * jnp.mean(scaled * unit_rows, axis=-1, keepdims=True)
    )
    return (inner_sum * inverse, jnp.sum(gradient * unit_rows, axis=0), jnp.sum(gradient, axis=0))


def masked_scores(rows_q, key_heads, first_row, score_scale):
    scores = (
        jnp.einsum("qgd,kgd->gqk", rows_q, key_heads, preferred_element_type=jnp.float32)
        * score_scale
    )
    place_q = first_row + jnp.arange(rows_q.shape[0], dtype=jnp.int32)
    place_k = jnp.arange(key_heads.shape[0], dtype=jnp.int32)
    allowed = place_k[None, :] <= place_q[:, None]
    return jnp.where(allowed[None], scores, -1e30)


def attend(queries, key_rows, value_rows, block_rows):
    length, width = queries.shape
    groups = width // HD
    score_scale = 1.0 / math.sqrt(HD)
    query_heads = queries.reshape(length, groups, HD)
    key_heads = key_rows.reshape(length, groups, HD)
    value_heads = value_rows.reshape(length, groups, HD)
    out_blocks = []
    totals = []
    for position in range(length // block_rows):
        first_row = position * block_rows
        last_row = first_row + block_rows
        scores = masked_scores(
            query_heads[first_row:last_row], key_heads[:last_row], first_row, score_scale
        )
        row_max = jnp.max(scores, axis=-1, keepdims=True)
        exp_scores = jnp.exp(scores - row_max)
        row_total = jnp.sum(exp_scores, axis=-1, keepdims=True)
        weights = (exp_scores / row_total).astype(jnp.bfloat16)
        out_blocks.append(
            jnp.einsum(
                "gqk,kgd->qgd", weights, value_heads[:last_row], preferred_element_type=jnp.float32
            )
        )
        totals.append(row_max + jnp.log(row_total))
    return (jnp.concatenate(out_blocks, axis=0).reshape(length, width), totals)


def attend_back(queries, key_rows, value_rows, grad_rows, totals, block_rows, first):
    length, width = queries.shape
    groups = width // HD
    score_scale = 1.0 / math.sqrt(HD)
    query_heads = queries.reshape(length, groups, HD)
    key_heads = key_rows.reshape(length, groups, HD)
    value_heads = value_rows.reshape(length, groups, HD)
    grad_heads = grad_rows.reshape(length, groups, HD)
    grad_keys = jnp.zeros((length, groups, HD), jnp.float32)
    grad_values = jnp.zeros((length, groups, HD), jnp.float32)
    query_parts = []
    for position in range(length // block_rows):
        first_row = position * block_rows
        last_row = first_row + block_rows
        rows_q = query_heads[first_row:last_row]
        if last_row == length:
            rows_q, grad_rows = lax.optimization_barrier(((rows_q, grad_heads), first))[0]
            grad_heads = grad_rows
        scores = masked_scores(rows_q, key_heads[:last_row], first_row, score_scale)
        weights = jnp.exp(scores - totals[position])
        rounded = weights.astype(jnp.bfloat16)
        grad_block = grad_heads[first_row:last_row]
        grad_values = grad_values.at[:last_row].add(
            jnp.einsum("gqk,qgd->kgd", rounded, grad_block, preferred_element_type=jnp.float32)
        )
        grad_weights = jnp.einsum(
            "qgd,kgd->gqk", grad_block, value_heads[:last_row], preferred_element_type=jnp.float32
        )
        inner_sum = jnp.sum(weights * grad_weights, axis=-1, keepdims=True)
        grad_scores = (weights * (grad_weights - inner_sum)).astype(jnp.bfloat16)
        query_parts.append(
            jnp.einsum(
                "gqk,kgd->qgd",
                grad_scores,
                key_heads[:last_row],
                preferred_element_type=jnp.float32,
            )
            * score_scale
        )
        grad_keys = grad_keys.at[:last_row].add(
            jnp.einsum("gqk,qgd->kgd", grad_scores, rows_q, preferred_element_type=jnp.float32)
            * score_scale
        )
    grad_queries = jnp.concatenate(query_parts, axis=0).reshape(length, width).astype(jnp.bfloat16)
    return (
        grad_queries,
        grad_keys.reshape(length, width).astype(jnp.bfloat16),
        grad_values.reshape(length, width).astype(jnp.bfloat16),
    )


def contract_rows(left_op, right_op):
    return lax.dot_general(
        left_op, right_op, (((0,), (0,)), ((), ())), preferred_element_type=jnp.float32
    )


def contract_cols(left_op, right_op):
    return lax.dot_general(
        left_op, right_op, (((1,), (1,)), ((), ())), preferred_element_type=jnp.float32
    )


WIDE = ("outer", "pair")
ALL = ("outer", "pair", "head")
LINE = ("pair", "head")
HEADS = 4


def swap(values):
    return lax.ppermute(values, "pair", [(0, 1), (1, 0)])


def send(values, moves):
    return lax.ppermute(values, LINE, [(a * HEADS + b, c * HEADS + d) for (a, b), (c, d) in moves])


def both(moves):
    return [((p, a), (p, b)) for p in range(2) for a, b in moves]


def shift(values, step):
    return lax.ppermute(values, "head", [(i, (i + step) % HEADS) for i in range(HEADS)])


def halves(block, axis):
    size = block.shape[axis] // 2
    place = lax.axis_index("pair")
    own = lax.dynamic_slice_in_dim(block, place * size, size, axis)
    other = lax.dynamic_slice_in_dim(block, (1 - place) * size, size, axis)
    return own, other


def in_order(own, other, axis):
    place = lax.axis_index("pair")
    return jnp.where(
        place == 0,
        jnp.concatenate([own, other], axis=axis),
        jnp.concatenate([other, own], axis=axis),
    )


def after(values, earlier):
    return lax.optimization_barrier((values, earlier))[0]


def spread(block):
    return [block] + [shift(block, k) for k in range(1, HEADS)]


def collect(blocks):
    total = blocks[0].astype(jnp.float32)
    for k in range(1, HEADS):
        total = total + shift(blocks[k], -k).astype(jnp.float32)
    return total


def half_rows(block):
    own, other = halves(block, 1)
    return in_order(own, swap(other), 0)


def scatter_half(rows):
    block = collect(jnp.split(rows, HEADS, axis=1)).astype(jnp.bfloat16)
    own, other = halves(block, 0)
    return in_order(own, swap(other), 1).astype(jnp.float32)


FORWARD = [((z // 2, z), (1 - z // 2, z)) for z in range(HEADS)]


def sequence_rows(block):
    place = lax.axis_index("head")
    holds = lax.axis_index("pair") == place // 2
    inner = (place == 1) | (place == 2)
    near = send(
        block,
        [((0, 0), (0, 1)), ((0, 1), (0, 0)), ((1, 2), (1, 3)), ((1, 3), (1, 2))],
    )
    next_in = send(block, [((0, 2), (0, 1)), ((1, 1), (1, 2))])
    last_in = send(block, [((0, 3), (0, 1)), ((1, 0), (1, 2))])
    outward = [((0, 1), (0, 0)), ((1, 2), (1, 3))]
    next_out = send(next_in, outward)
    last_out = send(last_in, outward)
    pieces = (
        block,
        near,
        jnp.where(inner, next_in, next_out),
        jnp.where(inner, last_in, last_out),
    )
    passed = [send(v, FORWARD) for v in pieces]
    own, near, following, last = (jnp.where(holds, v, w) for v, w in zip(pieces, passed))
    first = jnp.where(place % 2 == 0, own, near)
    second = jnp.where(place % 2 == 0, near, own)
    low = place < 2
    joined = jnp.concatenate(
        [
            jnp.where(low, first, last),
            jnp.where(low, second, following),
            jnp.where(low, following, first),
            jnp.where(low, last, second),
        ],
        axis=0,
    )
    return joined


def sequence_sum(partial):
    place = lax.axis_index("head")
    low = place < 2
    inner = jnp.where((place == 1) | (place == 2), 1, 0)
    rows = partial.shape[0] // HEADS
    bf16 = jnp.bfloat16

    def block(i):
        index = jnp.where(low, i, HEADS - 1 - i)
        piece = lax.dynamic_slice_in_dim(partial, index * rows, rows, 0)
        own, other = lax.optimization_barrier(halves(piece, 1))
        return own.astype(jnp.float32) + swap(other).astype(jnp.float32)

    inward = both([(0, 1), (3, 2)])
    near_moves = both([(0, 1), (1, 0), (2, 3), (3, 2)])
    last = block(3)
    last_in = send(last.astype(bf16), inward)
    following = block(2)
    following_in = send(following.astype(bf16), inward)
    away_in = send(block(1 - inner).astype(bf16), near_moves)
    mine = block(inner)
    last = (last + last_in.astype(jnp.float32)).astype(bf16)
    last = send(last, both([(1, 3), (2, 0)]))
    following = (following + following_in.astype(jnp.float32)).astype(bf16)
    following = send(following, both([(1, 2), (2, 1)]))
    return mine, away_in, following, last


def sequence_end(mine, away_in, following, last):
    place = lax.axis_index("head")
    inner = (place == 1) | (place == 2)
    mine = mine + away_in.astype(jnp.float32)
    far = jnp.where(inner, following, last).astype(jnp.float32)
    keeps = lax.axis_index("pair") == place // 2
    kept = jnp.where(keeps, mine, far)
    given = swap(jnp.where(keeps, far, mine).astype(jnp.bfloat16)).astype(jnp.float32)
    return in_order(kept, given, 1)


def group_moves(k):
    moves = []
    for p in range(2):
        for z in range(HEADS):
            group = 2 * (z % 2) + p
            moves.append(((p, z), (z // 2, (group + k) % HEADS)))
    return moves


def column_moves(k):
    moves = []
    for p in range(2):
        for group in range(HEADS):
            moves.append(((p, group), (group % 2, group // 2 + 2 * (p ^ k))))
    return moves


def turned(moves):
    return [(b, a) for a, b in moves]


def group_to_rows(values):
    rows = values.shape[0] // HEADS
    group = 2 * (lax.axis_index("head") % 2) + lax.axis_index("pair")
    parts = []
    for k in range(HEADS):
        start = (group + k) % HEADS * rows
        parts.append(send(lax.dynamic_slice_in_dim(values, start, rows, 0), group_moves(k)))
    return jnp.concatenate(parts, axis=1)


def rows_to_group(values):
    odd = lax.axis_index("pair") == 1
    upper = lax.axis_index("head") % 2 == 1
    parts = [
        send(part, turned(group_moves(k)))
        for k, part in enumerate(jnp.split(values, HEADS, axis=1))
    ]
    parts = [jnp.where(odd, parts[k - 1], parts[k]) for k in range(HEADS)]
    return jnp.concatenate(
        [jnp.where(upper, parts[k - 2], parts[k]) for k in range(HEADS)], axis=0
    )


def sum_all(values):
    for axis in ALL:
        size = lax.axis_size(axis)
        step = 1
        while step < size:
            values = values + lax.ppermute(values, axis, [(i, i ^ step) for i in range(size)])
            step *= 2
    return values


def layer(
    tokens, cotangent, w_query, w_key, w_value, w_out, w_up, w_down, norm_gain, norm_bias
):
    rows = tokens.shape[0]
    width = w_query.shape[1]
    model = w_query.shape[0] * lax.axis_size("outer") * 2
    bf16 = jnp.bfloat16
    f32 = jnp.float32
    late = lax.axis_index("head") // 2
    residual = tokens.astype(f32)
    norm_a, unit_a, inv_a = normalize(residual, norm_gain[0], norm_bias[0])

    w_cols = jnp.concatenate([w_query, w_key, w_value], axis=1)
    w_first, w_second = (send(w_cols, column_moves(k)) for k in range(2))
    w_cols = jnp.where(
        late == 0,
        jnp.concatenate([w_first, w_second], axis=0),
        jnp.concatenate([w_second, w_first], axis=0),
    )
    out_parts = spread(w_out.T)
    out_low = jnp.concatenate(out_parts[: HEADS // 2], axis=1)
    out_high = jnp.concatenate(out_parts[HEADS // 2 :], axis=1)
    attention = jnp.concatenate(
        [w_cols, jnp.concatenate([out_low, out_high], axis=0)], axis=1
    )
    attention = lax.all_gather(attention, "outer", axis=0, tiled=True)
    w_cols = attention[:, : 3 * width]
    out_own = attention[:, 3 * width :].reshape(-1, 2, w_out.shape[1], 2 * width)
    out_own = jnp.concatenate([out_own[:, 0], out_own[:, 1]], axis=2)
    seq_a = sequence_rows(norm_a.astype(bf16))
    up_block = half_rows(w_up)
    up_parts = spread(up_block)
    up_parts = jnp.concatenate(up_parts, axis=1)
    full_up = lax.all_gather(up_parts, "outer", axis=0, tiled=True)
    down_block = half_rows(w_down.T)
    down_parts = spread(down_block)

    block_rows = min(512, seq_a.shape[0])
    qkv = jnp.dot(seq_a, w_cols, preferred_element_type=f32).astype(bf16)
    down_parts = jnp.concatenate(down_parts, axis=1)
    full_down = lax.all_gather(down_parts, "outer", axis=0, tiled=True)
    queries, key_rows, value_rows = (qkv[:, i * width : (i + 1) * width] for i in range(3))
    attended, totals = attend(queries, key_rows, value_rows, block_rows)
    attended = group_to_rows(attended.astype(bf16))
    out_other = swap(out_own)
    place = lax.axis_index("pair")
    full_o = jnp.stack(
        [jnp.where(place == 0, out_own, out_other), jnp.where(place == 0, out_other, out_own)],
        axis=1,
    ).reshape(model, -1)
    mixed = contract_cols(attended, full_o)
    norm_z, unit_z, inv_z = normalize(mixed, norm_gain[1], norm_bias[1])
    hidden = residual + norm_z
    norm_c, unit_c, inv_c = normalize(hidden, norm_gain[2], norm_bias[2])
    rows_c = norm_c.astype(bf16)
    pair_c = jnp.concatenate([rows_c, swap(rows_c)], axis=0)
    pre_act = jnp.dot(pair_c, full_up, preferred_element_type=f32)
    active, gelu_back = jax.vjp(jax.nn.gelu, pre_act)
    active = active.astype(bf16)
    both_m = contract_cols(active, full_down)
    output = both_m[:rows] + swap(both_m[rows:].astype(bf16)).astype(f32)
    norm_m, unit_m, inv_m = normalize(output, norm_gain[3], norm_bias[3])
    block_out = (hidden + norm_m).astype(bf16)

    grad_y = cotangent.astype(f32)
    grad_m, gain_m, bias_m = normalize_back(grad_y, unit_m, inv_m, norm_gain[3])
    rows_gm = grad_m.astype(bf16)
    pair_gm = jnp.concatenate([rows_gm, swap(rows_gm)], axis=0)
    grad_act = jnp.dot(pair_gm, full_down, preferred_element_type=f32)
    grad_pre = gelu_back(grad_act)[0].astype(bf16)
    both_c = contract_cols(grad_pre, full_up)
    grad_c = both_c[:rows] + swap(both_c[rows:].astype(bf16)).astype(f32)
    grad_down = contract_rows(pair_gm, active).astype(bf16)
    grad_up = contract_rows(pair_c, grad_pre).astype(bf16)
    grad_more, gain_c, bias_c = normalize_back(grad_c, unit_c, inv_c, norm_gain[2])
    grad_h = grad_y + grad_more
    grad_z, gain_z, bias_z = normalize_back(grad_h, unit_z, inv_z, norm_gain[1])
    rows_gz = grad_z.astype(bf16)
    grad_att = jnp.dot(rows_gz, full_o, preferred_element_type=f32).astype(bf16)
    grad_att = rows_to_group(grad_att)
    grad_o = contract_rows(rows_gz, attended).astype(bf16)
    grad_o = grad_o.reshape(-1, 2, w_out.shape[1], attended.shape[1])
    own_o, other_o = halves(grad_o, 1)
    grad_o = (own_o.astype(f32) + swap(other_o).astype(f32)).astype(bf16)
    grad_o = grad_o.reshape(-1, attended.shape[1])
    grad_att = after(grad_att, (grad_down, grad_up, grad_o))
    grad_down = lax.psum_scatter(grad_down, "outer", scatter_dimension=0, tiled=True)
    grad_up = lax.psum_scatter(grad_up, "outer", scatter_dimension=0, tiled=True)
    grad_queries, grad_keys, grad_values = attend_back(
        queries, key_rows, value_rows, grad_att, totals, block_rows, (grad_down, grad_up)
    )
    grad_down = scatter_half(grad_down).T
    grad_up = scatter_half(grad_up)
    grad_qkv = jnp.concatenate([grad_queries, grad_keys, grad_values], axis=1)
    grad_qkv = after(grad_qkv, (grad_down, grad_up))
    grad_a = contract_cols(grad_qkv, w_cols).astype(bf16)
    grad_w = contract_rows(seq_a, after(grad_qkv, grad_a)).astype(bf16)
    grad_a = sequence_sum(grad_a)
    grad_o = grad_o.reshape(-1, 1, w_out.shape[1], attended.shape[1])
    grad_o = jnp.concatenate(jnp.split(grad_o, 2, axis=3), axis=1).reshape(model, -1)
    grad_w = jnp.concatenate([grad_w, grad_o], axis=1)
    grad_w = lax.psum_scatter(grad_w, "outer", scatter_dimension=0, tiled=True)
    landed = grad_w
    grad_w, grad_o = grad_w[:, : 3 * width], grad_w[:, 3 * width :]
    grad_o = collect(
        [
            grad_o[i * w_out.shape[1] : (i + 1) * w_out.shape[1], j * width : (j + 1) * width]
            for i in range(2)
            for j in range(2)
        ]
    ).T
    size = grad_w.shape[0] // 2
    parts = [
        send(
            lax.dynamic_slice_in_dim(grad_w, jnp.where(late == k, 0, size), size, 0),
            turned(column_moves(k)),
        ).astype(f32)
        for k in range(2)
    ]
    grad_w = parts[0] + parts[1]
    grad_a = sequence_end(*grad_a[:2], *after(grad_a[2:], landed))
    grad_first, gain_a, bias_a = normalize_back(grad_a, unit_a, inv_a, norm_gain[0])
    input_grad = grad_h + grad_first
    sums = sum_all(jnp.stack([gain_a, gain_z, gain_c, gain_m, bias_a, bias_z, bias_c, bias_m]))
    return (
        block_out,
        input_grad,
        grad_w[:, :width],
        grad_w[:, width : 2 * width],
        grad_w[:, 2 * width :],
        grad_o,
        grad_up,
        grad_down,
        sums[:4],
        sums[4:],
    )


def solution(mesh):
    wide, head = mesh.shape["wide"], mesh.shape["head"]
    assert head == HEADS and wide % 2 == 0
    paired = Mesh(mesh.devices.reshape(wide // 2, 2, head), ALL)
    rows = P(ALL, None)
    by_rows = P(WIDE, "head")
    by_cols = P("head", WIDE)
    in_specs = (rows, rows, by_rows, by_rows, by_rows, by_cols, by_rows, by_cols, P(), P())
    out_specs = (rows, rows, by_rows, by_rows, by_rows, by_cols, by_rows, by_cols, P(), P())
    return jax.shard_map(
        layer, mesh=paired, in_specs=in_specs, out_specs=out_specs, check_vma=False
    )
```

```python
import math

import jax
import jax.numpy as jnp
from jax import lax
from jax.experimental import pallas as pl
from jax.experimental.pallas import tpu as pltpu
from jax.sharding import Mesh, PartitionSpec as P


HD = 64


EPS = 1e-05


def normalize(values, gain, bias):
    average = jnp.mean(values, axis=-1, keepdims=True)
    centred = values - average
    inverse = lax.rsqrt(jnp.mean(centred * centred, axis=-1, keepdims=True) + EPS)
    unit_rows = centred * inverse
    return (unit_rows * gain + bias, unit_rows, inverse)


def normalize_back(gradient, unit_rows, inverse, gain):
    scaled = gradient * gain
    inner_sum = (
        scaled
        - jnp.mean(scaled, axis=-1, keepdims=True)
        - unit_rows * jnp.mean(scaled * unit_rows, axis=-1, keepdims=True)
    )
    return (inner_sum * inverse, jnp.sum(gradient * unit_rows, axis=0), jnp.sum(gradient, axis=0))


def head_lanes(shape, head):
    lane = lax.broadcasted_iota(jnp.int32, shape, 1)
    return (lane >= head * HD) & (lane < (head + 1) * HD)


def causal(shape):
    key = lax.broadcasted_iota(jnp.int32, shape, 0)
    query = lax.broadcasted_iota(jnp.int32, shape, 1)
    return key <= query


NT = (((1,), (1,)), ((), ()))


def attend_kernel(q_ref, k_ref, vt_ref, out_ref, total_ref, acc_ref):
    block, width = q_ref.shape
    position = pl.program_id(0)
    scaled = q_ref[...] * jnp.asarray(1.0 / math.sqrt(HD), jnp.bfloat16)
    heads = [
        jnp.where(head_lanes((block, width), h), scaled, jnp.zeros_like(scaled))
        for h in range(width // HD)
    ]

    def scores(h, j):
        start = pl.multiple_of(j * block, block)
        keys = k_ref[pl.ds(start, block), :]
        return lax.dot_general(keys, heads[h], NT, preferred_element_type=jnp.float32)

    def mix(h, j, weights):
        start = pl.multiple_of(j * block, block)
        values = vt_ref[h * HD : (h + 1) * HD, pl.ds(start, block)]
        return jnp.dot(values, weights.astype(jnp.bfloat16), preferred_element_type=jnp.float32)

    first = []
    for h in range(width // HD):
        s = jnp.where(causal((block, block)), scores(h, position), -1e30)
        top = jnp.max(s, axis=0, keepdims=True)
        p = jnp.exp(s - top)
        first += [top, jnp.sum(p, axis=0, keepdims=True)]
        acc_ref[h * HD : (h + 1) * HD, :] = mix(h, position, p)

    def step(j, carry):
        carry = list(carry)
        for h in range(width // HD):
            s = scores(h, j)
            top = jnp.maximum(carry[2 * h], jnp.max(s, axis=0, keepdims=True))
            p = jnp.exp(s - top)
            old = jnp.exp(carry[2 * h] - top)
            carry[2 * h + 1] = carry[2 * h + 1] * old + jnp.sum(p, axis=0, keepdims=True)
            carry[2 * h] = top
            rows = slice(h * HD, (h + 1) * HD)
            acc_ref[rows, :] = acc_ref[rows, :] * old + mix(h, j, p)
        return tuple(carry)

    last = lax.fori_loop(0, position, step, tuple(first))
    for h in range(width // HD):
        rows = slice(h * HD, (h + 1) * HD)
        acc_ref[rows, :] = acc_ref[rows, :] / last[2 * h + 1]
        total_ref[h : h + 1, :] = last[2 * h] + jnp.log(last[2 * h + 1])
    out_ref[...] = acc_ref[...].T.astype(jnp.bfloat16)


def attend(qkv, turned_kv, block):
    length, width = qkv.shape[0], qkv.shape[1] // 3
    return pl.pallas_call(
        attend_kernel,
        grid=(length // block,),
        in_specs=[
            pl.BlockSpec((block, width), lambda i: (i, 0)),
            pl.BlockSpec((length, width), lambda i: (0, 1)),
            pl.BlockSpec((width, length), lambda i: (1, 0)),
        ],
        out_specs=[
            pl.BlockSpec((block, width), lambda i: (i, 0)),
            pl.BlockSpec((width // HD, block), lambda i: (0, i)),
        ],
        out_shape=[
            jax.ShapeDtypeStruct((length, width), jnp.bfloat16),
            jax.ShapeDtypeStruct((width // HD, length), jnp.float32),
        ],
        scratch_shapes=[pltpu.VMEM((width, block), jnp.float32)],
        name="attend",
    )(qkv, qkv, turned_kv)


def attend_back_kernel(
    q_ref, k_ref, v_ref, kt_ref, grad_ref, out_ref, total_ref, back_ref, dq_ref, dk_ref, dv_ref
):
    block, width = q_ref.shape
    position = pl.program_id(0)
    score_scale = 1.0 / math.sqrt(HD)

    @pl.when(position == 0)
    def _():
        dk_ref[...] = jnp.zeros_like(dk_ref)
        dv_ref[...] = jnp.zeros_like(dv_ref)

    dq_ref[...] = jnp.zeros_like(dq_ref)
    scaled = q_ref[...] * jnp.asarray(score_scale, jnp.bfloat16)
    grads = grad_ref[...]
    zero = jnp.zeros_like(scaled)
    query_heads = [
        jnp.where(head_lanes((block, width), h), scaled, zero) for h in range(width // HD)
    ]
    grad_heads = [
        jnp.where(head_lanes((block, width), h), grads, zero) for h in range(width // HD)
    ]
    shared = (grads.astype(jnp.float32) * out_ref[...].astype(jnp.float32)).T
    inner = [
        jnp.sum(shared[h * HD : (h + 1) * HD, :], axis=0, keepdims=True)
        for h in range(width // HD)
    ]

    def chunk(j, masked):
        rows = pl.ds(pl.multiple_of(j * block, block), block)
        keys = k_ref[rows, :]
        values = v_ref[rows, :]
        dk = dk_ref[rows, :]
        dv = dv_ref[rows, :]
        for h in range(width // HD):
            s = lax.dot_general(keys, query_heads[h], NT, preferred_element_type=jnp.float32)
            p = jnp.exp(s - total_ref[h : h + 1, :])
            if masked:
                p = jnp.where(causal((block, block)), p, 0.0)
            dp = lax.dot_general(values, grad_heads[h], NT, preferred_element_type=jnp.float32)
            ds = (p * (dp - inner[h])).astype(jnp.bfloat16)
            dv += jnp.dot(
                p.astype(jnp.bfloat16), grad_heads[h], preferred_element_type=jnp.float32
            )
            dk += jnp.dot(ds, query_heads[h], preferred_element_type=jnp.float32)
            lanes = slice(h * HD, (h + 1) * HD)
            dq_ref[lanes, :] += jnp.dot(
                kt_ref[lanes, rows], ds, preferred_element_type=jnp.float32
            )
        dk_ref[rows, :] = dk
        dv_ref[rows, :] = dv

    def step(j, carry):
        chunk(j, False)
        return carry

    lax.fori_loop(0, position, step, 0)
    chunk(position, True)
    rows = pl.ds(pl.multiple_of(position * block, block), block)
    back_ref[rows, :width] = (dq_ref[...] * score_scale).T.astype(jnp.bfloat16)

    @pl.when(position == pl.num_programs(0) - 1)
    def _():
        back_ref[:, width : 2 * width] = dk_ref[...].astype(jnp.bfloat16)
        back_ref[:, 2 * width :] = dv_ref[...].astype(jnp.bfloat16)


def attend_back(qkv, turned_kv, grad_rows, attended, totals, block):
    length, width = grad_rows.shape
    return pl.pallas_call(
        attend_back_kernel,
        grid=(length // block,),
        in_specs=[
            pl.BlockSpec((block, width), lambda i: (i, 0)),
            pl.BlockSpec((length, width), lambda i: (0, 1)),
            pl.BlockSpec((length, width), lambda i: (0, 2)),
            pl.BlockSpec((width, length), lambda i: (0, 0)),
            pl.BlockSpec((block, width), lambda i: (i, 0)),
            pl.BlockSpec((block, width), lambda i: (i, 0)),
            pl.BlockSpec((width // HD, block), lambda i: (0, i)),
        ],
        out_specs=pl.BlockSpec((length, 3 * width), lambda i: (0, 0)),
        out_shape=jax.ShapeDtypeStruct((length, 3 * width), jnp.bfloat16),
        scratch_shapes=[
            pltpu.VMEM((width, block), jnp.float32),
            pltpu.VMEM((length, width), jnp.float32),
            pltpu.VMEM((length, width), jnp.float32),
        ],
        name="attend_back",
    )(qkv, qkv, qkv, turned_kv, grad_rows, attended, totals)


def contract_rows(left_op, right_op):
    return lax.dot_general(
        left_op, right_op, (((0,), (0,)), ((), ())), preferred_element_type=jnp.float32
    )


def contract_cols(left_op, right_op):
    return lax.dot_general(
        left_op, right_op, (((1,), (1,)), ((), ())), preferred_element_type=jnp.float32
    )


WIDE = ("outer", "pair")
ALL = ("outer", "pair", "head")
LINE = ("pair", "head")
HEADS = 4


def swap(values):
    return lax.ppermute(values, "pair", [(0, 1), (1, 0)])


def send(values, moves):
    return lax.ppermute(values, LINE, [(a * HEADS + b, c * HEADS + d) for (a, b), (c, d) in moves])


def both(moves):
    return [((p, a), (p, b)) for p in range(2) for a, b in moves]


def shift(values, step):
    return lax.ppermute(values, "head", [(i, (i + step) % HEADS) for i in range(HEADS)])


def halves(block, axis):
    size = block.shape[axis] // 2
    place = lax.axis_index("pair")
    own = lax.dynamic_slice_in_dim(block, place * size, size, axis)
    other = lax.dynamic_slice_in_dim(block, (1 - place) * size, size, axis)
    return own, other


def in_order(own, other, axis):
    place = lax.axis_index("pair")
    return jnp.where(
        place == 0,
        jnp.concatenate([own, other], axis=axis),
        jnp.concatenate([other, own], axis=axis),
    )


def after(values, earlier):
    return lax.optimization_barrier((values, earlier))[0]


def spread(block):
    return [block] + [shift(block, k) for k in range(1, HEADS)]


def collect(blocks):
    total = blocks[0].astype(jnp.float32)
    for k in range(1, HEADS):
        total = total + shift(blocks[k], -k).astype(jnp.float32)
    return total


def half_rows(block):
    own, other = halves(block, 1)
    return in_order(own, swap(other), 0)


def scatter_half(rows):
    block = collect(jnp.split(rows, HEADS, axis=1)).astype(jnp.bfloat16)
    own, other = halves(block, 0)
    return in_order(own, swap(other), 1).astype(jnp.float32)


FORWARD = [((z // 2, z), (1 - z // 2, z)) for z in range(HEADS)]


def sequence_rows(block):
    place = lax.axis_index("head")
    holds = lax.axis_index("pair") == place // 2
    inner = (place == 1) | (place == 2)
    near = send(
        block,
        [((0, 0), (0, 1)), ((0, 1), (0, 0)), ((1, 2), (1, 3)), ((1, 3), (1, 2))],
    )
    next_in = send(block, [((0, 2), (0, 1)), ((1, 1), (1, 2))])
    last_in = send(block, [((0, 3), (0, 1)), ((1, 0), (1, 2))])
    outward = [((0, 1), (0, 0)), ((1, 2), (1, 3))]
    next_out = send(next_in, outward)
    last_out = send(last_in, outward)
    pieces = (
        block,
        near,
        jnp.where(inner, next_in, next_out),
        jnp.where(inner, last_in, last_out),
    )
    passed = [send(v, FORWARD) for v in pieces]
    own, near, following, last = (jnp.where(holds, v, w) for v, w in zip(pieces, passed))
    first = jnp.where(place % 2 == 0, own, near)
    second = jnp.where(place % 2 == 0, near, own)
    low = place < 2
    joined = jnp.concatenate(
        [
            jnp.where(low, first, last),
            jnp.where(low, second, following),
            jnp.where(low, following, first),
            jnp.where(low, last, second),
        ],
        axis=0,
    )
    return joined


def sequence_sum(partial):
    place = lax.axis_index("head")
    low = place < 2
    inner = jnp.where((place == 1) | (place == 2), 1, 0)
    rows = partial.shape[0] // HEADS
    bf16 = jnp.bfloat16

    def block(i):
        index = jnp.where(low, i, HEADS - 1 - i)
        piece = lax.dynamic_slice_in_dim(partial, index * rows, rows, 0)
        own, other = lax.optimization_barrier(halves(piece, 1))
        return own.astype(jnp.float32) + swap(other).astype(jnp.float32)

    inward = both([(0, 1), (3, 2)])
    near_moves = both([(0, 1), (1, 0), (2, 3), (3, 2)])
    last = block(3)
    last_in = send(last.astype(bf16), inward)
    following = block(2)
    following_in = send(following.astype(bf16), inward)
    away = block(1 - inner).astype(bf16)
    away_in = send(away, near_moves)
    mine = block(inner)
    last = (last + last_in.astype(jnp.float32)).astype(bf16)
    last = send(last, both([(1, 3), (2, 0)]))
    following = (following + following_in.astype(jnp.float32)).astype(bf16)
    following = send(following, both([(1, 2), (2, 1)]))
    return mine, away_in, following, last


def sequence_end(mine, away_in, following, last):
    place = lax.axis_index("head")
    inner = (place == 1) | (place == 2)
    mine = mine + away_in.astype(jnp.float32)
    far = jnp.where(inner, following, last).astype(jnp.float32)
    keeps = lax.axis_index("pair") == place // 2
    kept = jnp.where(keeps, mine, far)
    given = jnp.where(keeps, far, mine).astype(jnp.bfloat16)
    given = swap(given)
    given = given.astype(jnp.float32)
    return in_order(kept, given, 1)


def group_moves(k):
    moves = []
    for p in range(2):
        for z in range(HEADS):
            group = 2 * (z % 2) + p
            moves.append(((p, z), (z // 2, (group + k) % HEADS)))
    return moves


def column_moves(k):
    moves = []
    for p in range(2):
        for group in range(HEADS):
            moves.append(((p, group), (group % 2, group // 2 + 2 * (p ^ k))))
    return moves


def turned(moves):
    return [(b, a) for a, b in moves]


def group_to_rows(values):
    rows = values.shape[0] // HEADS
    group = 2 * (lax.axis_index("head") % 2) + lax.axis_index("pair")
    parts = []
    for k in range(HEADS):
        start = (group + k) % HEADS * rows
        parts.append(send(lax.dynamic_slice_in_dim(values, start, rows, 0), group_moves(k)))
    return jnp.concatenate(parts, axis=1)


def rows_to_group(values):
    odd = lax.axis_index("pair") == 1
    upper = lax.axis_index("head") % 2 == 1
    parts = [
        send(part, turned(group_moves(k)))
        for k, part in enumerate(jnp.split(values, HEADS, axis=1))
    ]
    parts = [jnp.where(odd, parts[k - 1], parts[k]) for k in range(HEADS)]
    return jnp.concatenate(
        [jnp.where(upper, parts[k - 2], parts[k]) for k in range(HEADS)], axis=0
    )


def sum_all(values):
    for axis in ALL:
        size = lax.axis_size(axis)
        step = 1
        while step < size:
            values = values + lax.ppermute(values, axis, [(i, i ^ step) for i in range(size)])
            step *= 2
    return values


def layer(
    tokens, cotangent, w_query, w_key, w_value, w_out, w_up, w_down, norm_gain, norm_bias
):
    rows = tokens.shape[0]
    width = w_query.shape[1]
    model = w_query.shape[0] * lax.axis_size("outer") * 2
    bf16 = jnp.bfloat16
    f32 = jnp.float32
    late = lax.axis_index("head") // 2
    residual = tokens.astype(f32)
    norm_a, unit_a, inv_a = normalize(residual, norm_gain[0], norm_bias[0])

    w_cols = jnp.concatenate([w_query, w_key, w_value], axis=1)
    w_first, w_second = (send(w_cols, column_moves(k)) for k in range(2))
    w_cols = jnp.where(
        late == 0,
        jnp.concatenate([w_first, w_second], axis=0),
        jnp.concatenate([w_second, w_first], axis=0),
    )
    out_parts = spread(w_out.T)
    out_low = jnp.concatenate(out_parts[: HEADS // 2], axis=1)
    out_high = jnp.concatenate(out_parts[HEADS // 2 :], axis=1)
    attention = jnp.concatenate(
        [w_cols, jnp.concatenate([out_low, out_high], axis=0)], axis=1
    )
    attention = lax.all_gather(attention, "outer", axis=0, tiled=True)
    w_cols = attention[:, : 3 * width]
    out_own = attention[:, 3 * width :].reshape(-1, 2, w_out.shape[1], 2 * width)
    out_own = jnp.concatenate([out_own[:, 0], out_own[:, 1]], axis=2)
    seq_a = sequence_rows(norm_a.astype(bf16))
    up_block = half_rows(w_up)
    up_parts = spread(up_block)
    up_parts = jnp.concatenate(up_parts, axis=1)
    full_up = lax.all_gather(up_parts, "outer", axis=0, tiled=True)
    down_block = half_rows(w_down.T)
    down_parts = spread(down_block)

    block_rows = min(512, seq_a.shape[0])
    qkv = jnp.dot(seq_a, w_cols, preferred_element_type=f32).astype(bf16)
    down_parts = jnp.concatenate(down_parts, axis=1)
    full_down = lax.all_gather(down_parts, "outer", axis=0, tiled=True)
    turned_kv = qkv[:, width:].T
    seen, totals = attend(qkv, turned_kv, block_rows)
    attended = group_to_rows(seen)
    out_other = swap(out_own)
    place = lax.axis_index("pair")
    full_o = jnp.stack(
        [jnp.where(place == 0, out_own, out_other), jnp.where(place == 0, out_other, out_own)],
        axis=1,
    ).reshape(model, -1)
    mixed = contract_cols(attended, full_o)
    norm_z, unit_z, inv_z = normalize(mixed, norm_gain[1], norm_bias[1])
    hidden = residual + norm_z
    norm_c, unit_c, inv_c = normalize(hidden, norm_gain[2], norm_bias[2])
    rows_c = norm_c.astype(bf16)
    pair_c = jnp.concatenate([rows_c, swap(rows_c)], axis=0)
    pre_act = jnp.dot(pair_c, full_up, preferred_element_type=f32)
    active, gelu_back = jax.vjp(jax.nn.gelu, pre_act)
    active = active.astype(bf16)
    both_m = contract_cols(active, full_down)
    output = both_m[:rows] + swap(both_m[rows:].astype(bf16)).astype(f32)
    norm_m, unit_m, inv_m = normalize(output, norm_gain[3], norm_bias[3])
    block_out = (hidden + norm_m).astype(bf16)

    grad_y = cotangent.astype(f32)
    grad_m, gain_m, bias_m = normalize_back(grad_y, unit_m, inv_m, norm_gain[3])
    rows_gm = grad_m.astype(bf16)
    pair_gm = jnp.concatenate([rows_gm, swap(rows_gm)], axis=0)
    grad_act = jnp.dot(pair_gm, full_down, preferred_element_type=f32)
    grad_pre = gelu_back(grad_act)[0].astype(bf16)
    both_c = contract_cols(grad_pre, full_up)
    grad_c = both_c[:rows] + swap(both_c[rows:].astype(bf16)).astype(f32)
    grad_down = contract_rows(pair_gm, active).astype(bf16)
    grad_up = contract_rows(pair_c, grad_pre).astype(bf16)
    grad_more, gain_c, bias_c = normalize_back(grad_c, unit_c, inv_c, norm_gain[2])
    grad_h = grad_y + grad_more
    grad_z, gain_z, bias_z = normalize_back(grad_h, unit_z, inv_z, norm_gain[1])
    rows_gz = grad_z.astype(bf16)
    grad_att = jnp.dot(rows_gz, full_o, preferred_element_type=f32).astype(bf16)
    grad_att = rows_to_group(grad_att)
    grad_o = contract_rows(rows_gz, attended).astype(bf16)
    grad_o = grad_o.reshape(-1, 2, w_out.shape[1], attended.shape[1])
    own_o, other_o = halves(grad_o, 1)
    grad_o = (own_o.astype(f32) + swap(other_o).astype(f32)).astype(bf16)
    grad_o = grad_o.reshape(-1, attended.shape[1])
    grad_att = after(grad_att, (grad_down, grad_up, grad_o))
    grad_down = lax.psum_scatter(grad_down, "outer", scatter_dimension=0, tiled=True)
    grad_up = lax.psum_scatter(grad_up, "outer", scatter_dimension=0, tiled=True)
    grad_qkv = attend_back(qkv, turned_kv, grad_att, seen, totals, block_rows)
    grad_down = scatter_half(grad_down).T
    grad_up = scatter_half(grad_up)
    grad_a = contract_cols(grad_qkv, w_cols).astype(bf16)
    grad_w = contract_rows(seq_a, after(grad_qkv, grad_a)).astype(bf16)
    grad_a = sequence_sum(grad_a)
    grad_o = grad_o.reshape(-1, 1, w_out.shape[1], attended.shape[1])
    grad_o = jnp.concatenate(jnp.split(grad_o, 2, axis=3), axis=1).reshape(model, -1)
    grad_w = jnp.concatenate([grad_w, grad_o], axis=1)
    grad_w = lax.psum_scatter(grad_w, "outer", scatter_dimension=0, tiled=True)
    landed = grad_w
    grad_w, grad_o = grad_w[:, : 3 * width], grad_w[:, 3 * width :]
    grad_o = collect(
        [
            grad_o[i * w_out.shape[1] : (i + 1) * w_out.shape[1], j * width : (j + 1) * width]
            for i in range(2)
            for j in range(2)
        ]
    ).T
    size = grad_w.shape[0] // 2
    parts = [
        send(
            lax.dynamic_slice_in_dim(grad_w, jnp.where(late == k, 0, size), size, 0),
            turned(column_moves(k)),
        ).astype(f32)
        for k in range(2)
    ]
    grad_w = parts[0] + parts[1]
    grad_a = sequence_end(*grad_a[:2], *after(grad_a[2:], landed))
    grad_first, gain_a, bias_a = normalize_back(grad_a, unit_a, inv_a, norm_gain[0])
    input_grad = grad_h + grad_first
    sums = sum_all(jnp.stack([gain_a, gain_z, gain_c, gain_m, bias_a, bias_z, bias_c, bias_m]))
    return (
        block_out,
        input_grad,
        grad_w[:, :width],
        grad_w[:, width : 2 * width],
        grad_w[:, 2 * width :],
        grad_o,
        grad_up,
        grad_down,
        sums[:4],
        sums[4:],
    )


def solution(mesh):
    wide, head = mesh.shape["wide"], mesh.shape["head"]
    assert head == HEADS and wide % 2 == 0
    paired = Mesh(mesh.devices.reshape(wide // 2, 2, head), ALL)
    rows = P(ALL, None)
    by_rows = P(WIDE, "head")
    by_cols = P("head", WIDE)
    in_specs = (rows, rows, by_rows, by_rows, by_rows, by_cols, by_rows, by_cols, P(), P())
    out_specs = (rows, rows, by_rows, by_rows, by_rows, by_cols, by_rows, by_cols, P(), P())
    return jax.shard_map(
        layer, mesh=paired, in_specs=in_specs, out_specs=out_specs, check_vma=False
    )
```

```python
import math

import jax
import jax.numpy as jnp
from jax import lax
from jax.experimental import pallas as pl
from jax.experimental.pallas import tpu as pltpu
from jax.sharding import Mesh, PartitionSpec as P


HD = 64


EPS = 1e-05


def normalize(values, gain, bias):
    average = jnp.mean(values, axis=-1, keepdims=True)
    centred = values - average
    inverse = lax.rsqrt(jnp.mean(centred * centred, axis=-1, keepdims=True) + EPS)
    unit_rows = centred * inverse
    return (unit_rows * gain + bias, unit_rows, inverse)


def normalize_back(gradient, unit_rows, inverse, gain):
    scaled = gradient * gain
    inner_sum = (
        scaled
        - jnp.mean(scaled, axis=-1, keepdims=True)
        - unit_rows * jnp.mean(scaled * unit_rows, axis=-1, keepdims=True)
    )
    return (inner_sum * inverse, jnp.sum(gradient * unit_rows, axis=0), jnp.sum(gradient, axis=0))


def head_lanes(shape, head):
    lane = lax.broadcasted_iota(jnp.int32, shape, 1)
    return (lane >= head * HD) & (lane < (head + 1) * HD)


def causal(shape):
    key = lax.broadcasted_iota(jnp.int32, shape, 0)
    query = lax.broadcasted_iota(jnp.int32, shape, 1)
    return key <= query


NT = (((1,), (1,)), ((), ()))


def attend_kernel(q_ref, k_ref, vt_ref, out_ref, total_ref, acc_ref):
    block, width = q_ref.shape
    position = pl.program_id(0)
    scaled = q_ref[...] * jnp.asarray(1.0 / math.sqrt(HD), jnp.bfloat16)
    heads = [
        jnp.where(head_lanes((block, width), h), scaled, jnp.zeros_like(scaled))
        for h in range(width // HD)
    ]

    def scores(h, j):
        start = pl.multiple_of(j * block, block)
        keys = k_ref[pl.ds(start, block), :]
        return lax.dot_general(keys, heads[h], NT, preferred_element_type=jnp.float32)

    def mix(h, j, weights):
        start = pl.multiple_of(j * block, block)
        values = vt_ref[h * HD : (h + 1) * HD, pl.ds(start, block)]
        return jnp.dot(values, weights.astype(jnp.bfloat16), preferred_element_type=jnp.float32)

    first = []
    for h in range(width // HD):
        s = jnp.where(causal((block, block)), scores(h, position), -1e30)
        top = jnp.max(s, axis=0, keepdims=True)
        p = jnp.exp(s - top)
        first += [top, jnp.sum(p, axis=0, keepdims=True)]
        acc_ref[h * HD : (h + 1) * HD, :] = mix(h, position, p)

    def step(j, carry):
        carry = list(carry)
        for h in range(width // HD):
            s = scores(h, j)
            top = jnp.maximum(carry[2 * h], jnp.max(s, axis=0, keepdims=True))
            p = jnp.exp(s - top)
            old = jnp.exp(carry[2 * h] - top)
            carry[2 * h + 1] = carry[2 * h + 1] * old + jnp.sum(p, axis=0, keepdims=True)
            carry[2 * h] = top
            rows = slice(h * HD, (h + 1) * HD)
            acc_ref[rows, :] = acc_ref[rows, :] * old + mix(h, j, p)
        return tuple(carry)

    last = lax.fori_loop(0, position, step, tuple(first))
    for h in range(width // HD):
        rows = slice(h * HD, (h + 1) * HD)
        acc_ref[rows, :] = acc_ref[rows, :] / last[2 * h + 1]
        total_ref[h : h + 1, :] = last[2 * h] + jnp.log(last[2 * h + 1])
    out_ref[...] = acc_ref[...].T.astype(jnp.bfloat16)


def attend(qkv, turned_kv, block):
    length, width = qkv.shape[0], qkv.shape[1] // 3
    return pl.pallas_call(
        attend_kernel,
        grid=(length // block,),
        in_specs=[
            pl.BlockSpec((block, width), lambda i: (i, 0)),
            pl.BlockSpec((length, width), lambda i: (0, 1)),
            pl.BlockSpec((width, length), lambda i: (1, 0)),
        ],
        out_specs=[
            pl.BlockSpec((block, width), lambda i: (i, 0)),
            pl.BlockSpec((width // HD, block), lambda i: (0, i)),
        ],
        out_shape=[
            jax.ShapeDtypeStruct((length, width), jnp.bfloat16),
            jax.ShapeDtypeStruct((width // HD, length), jnp.float32),
        ],
        scratch_shapes=[pltpu.VMEM((width, block), jnp.float32)],
        name="attend",
    )(qkv, qkv, turned_kv)


def attend_back_kernel(
    q_ref, k_ref, v_ref, kt_ref, grad_ref, out_ref, total_ref, back_ref, dq_ref, dk_ref, dv_ref
):
    block, width = q_ref.shape
    position = pl.program_id(0)
    score_scale = 1.0 / math.sqrt(HD)

    @pl.when(position == 0)
    def _():
        dk_ref[...] = jnp.zeros_like(dk_ref)
        dv_ref[...] = jnp.zeros_like(dv_ref)

    dq_ref[...] = jnp.zeros_like(dq_ref)
    scaled = q_ref[...] * jnp.asarray(score_scale, jnp.bfloat16)
    grads = grad_ref[...]
    zero = jnp.zeros_like(scaled)
    query_heads = [
        jnp.where(head_lanes((block, width), h), scaled, zero) for h in range(width // HD)
    ]
    grad_heads = [
        jnp.where(head_lanes((block, width), h), grads, zero) for h in range(width // HD)
    ]
    shared = (grads.astype(jnp.float32) * out_ref[...].astype(jnp.float32)).T
    inner = [
        jnp.sum(shared[h * HD : (h + 1) * HD, :], axis=0, keepdims=True)
        for h in range(width // HD)
    ]

    def chunk(j, masked):
        rows = pl.ds(pl.multiple_of(j * block, block), block)
        keys = k_ref[rows, :]
        values = v_ref[rows, :]
        dk = dk_ref[rows, :]
        dv = dv_ref[rows, :]
        for h in range(width // HD):
            s = lax.dot_general(keys, query_heads[h], NT, preferred_element_type=jnp.float32)
            p = jnp.exp(s - total_ref[h : h + 1, :])
            if masked:
                p = jnp.where(causal((block, block)), p, 0.0)
            dp = lax.dot_general(values, grad_heads[h], NT, preferred_element_type=jnp.float32)
            ds = (p * (dp - inner[h])).astype(jnp.bfloat16)
            dv += jnp.dot(
                p.astype(jnp.bfloat16), grad_heads[h], preferred_element_type=jnp.float32
            )
            dk += jnp.dot(ds, query_heads[h], preferred_element_type=jnp.float32)
            lanes = slice(h * HD, (h + 1) * HD)
            dq_ref[lanes, :] += jnp.dot(
                kt_ref[lanes, rows], ds, preferred_element_type=jnp.float32
            )
        dk_ref[rows, :] = dk
        dv_ref[rows, :] = dv

    def step(j, carry):
        chunk(j, False)
        return carry

    lax.fori_loop(0, position, step, 0)
    chunk(position, True)
    rows = pl.ds(pl.multiple_of(position * block, block), block)
    back_ref[rows, :width] = (dq_ref[...] * score_scale).T.astype(jnp.bfloat16)

    @pl.when(position == pl.num_programs(0) - 1)
    def _():
        back_ref[:, width : 2 * width] = dk_ref[...].astype(jnp.bfloat16)
        back_ref[:, 2 * width :] = dv_ref[...].astype(jnp.bfloat16)


def attend_back(qkv, turned_kv, grad_rows, attended, totals, block):
    length, width = grad_rows.shape
    return pl.pallas_call(
        attend_back_kernel,
        grid=(length // block,),
        in_specs=[
            pl.BlockSpec((block, width), lambda i: (i, 0)),
            pl.BlockSpec((length, width), lambda i: (0, 1)),
            pl.BlockSpec((length, width), lambda i: (0, 2)),
            pl.BlockSpec((width, length), lambda i: (0, 0)),
            pl.BlockSpec((block, width), lambda i: (i, 0)),
            pl.BlockSpec((block, width), lambda i: (i, 0)),
            pl.BlockSpec((width // HD, block), lambda i: (0, i)),
        ],
        out_specs=pl.BlockSpec((length, 3 * width), lambda i: (0, 0)),
        out_shape=jax.ShapeDtypeStruct((length, 3 * width), jnp.bfloat16),
        scratch_shapes=[
            pltpu.VMEM((width, block), jnp.float32),
            pltpu.VMEM((length, width), jnp.float32),
            pltpu.VMEM((length, width), jnp.float32),
        ],
        name="attend_back",
    )(qkv, qkv, qkv, turned_kv, grad_rows, attended, totals)


def contract_rows(left_op, right_op):
    return lax.dot_general(
        left_op, right_op, (((0,), (0,)), ((), ())), preferred_element_type=jnp.float32
    )


def contract_cols(left_op, right_op):
    return lax.dot_general(
        left_op, right_op, (((1,), (1,)), ((), ())), preferred_element_type=jnp.float32
    )


WIDE = ("outer", "pair")
ALL = ("outer", "pair", "head")
LINE = ("pair", "head")
HEADS = 4


def swap(values):
    return lax.ppermute(values, "pair", [(0, 1), (1, 0)])


def send(values, moves):
    return lax.ppermute(values, LINE, [(a * HEADS + b, c * HEADS + d) for (a, b), (c, d) in moves])


def both(moves):
    return [((p, a), (p, b)) for p in range(2) for a, b in moves]


def shift(values, step):
    return lax.ppermute(values, "head", [(i, (i + step) % HEADS) for i in range(HEADS)])


def halves(block, axis):
    size = block.shape[axis] // 2
    place = lax.axis_index("pair")
    own = lax.dynamic_slice_in_dim(block, place * size, size, axis)
    other = lax.dynamic_slice_in_dim(block, (1 - place) * size, size, axis)
    return own, other


def in_order(own, other, axis):
    place = lax.axis_index("pair")
    return jnp.where(
        place == 0,
        jnp.concatenate([own, other], axis=axis),
        jnp.concatenate([other, own], axis=axis),
    )


def after(values, earlier):
    return lax.optimization_barrier((values, earlier))[0]


def spread(block):
    return [block] + [shift(block, k) for k in range(1, HEADS)]


def collect(blocks):
    total = blocks[0].astype(jnp.float32)
    for k in range(1, HEADS):
        total = total + shift(blocks[k], -k).astype(jnp.float32)
    return total


def half_rows(block):
    own, other = halves(block, 1)
    other = swap(other)
    return in_order(own, other, 0)


def scatter_half(rows):
    block = collect(jnp.split(rows, HEADS, axis=1)).astype(jnp.bfloat16)
    own, other = halves(block, 0)
    return in_order(own, swap(other), 1).astype(jnp.float32)


FORWARD = [((z // 2, z), (1 - z // 2, z)) for z in range(HEADS)]


def sequence_rows(block):
    place = lax.axis_index("head")
    holds = lax.axis_index("pair") == place // 2
    inner = (place == 1) | (place == 2)
    near = send(
        block,
        [((0, 0), (0, 1)), ((0, 1), (0, 0)), ((1, 2), (1, 3)), ((1, 3), (1, 2))],
    )
    next_in = send(block, [((0, 2), (0, 1)), ((1, 1), (1, 2))])
    last_in = send(block, [((0, 3), (0, 1)), ((1, 0), (1, 2))])
    outward = [((0, 1), (0, 0)), ((1, 2), (1, 3))]
    next_out = send(next_in, outward)
    last_out = send(last_in, outward)
    pieces = (
        block,
        near,
        jnp.where(inner, next_in, next_out),
        jnp.where(inner, last_in, last_out),
    )
    passed = [send(v, FORWARD) for v in pieces]
    own, near, following, last = (jnp.where(holds, v, w) for v, w in zip(pieces, passed))
    first = jnp.where(place % 2 == 0, own, near)
    second = jnp.where(place % 2 == 0, near, own)
    low = place < 2
    joined = jnp.concatenate(
        [
            jnp.where(low, first, last),
            jnp.where(low, second, following),
            jnp.where(low, following, first),
            jnp.where(low, last, second),
        ],
        axis=0,
    )
    return joined


def sequence_sum(own_half, other_half):
    place = lax.axis_index("head")
    low = place < 2
    inner = jnp.where((place == 1) | (place == 2), 1, 0)
    rows = own_half.shape[0] // HEADS
    bf16 = jnp.bfloat16

    def block(i):
        index = jnp.where(low, i, HEADS - 1 - i)
        own = lax.dynamic_slice_in_dim(own_half, index * rows, rows, 0)
        other = lax.dynamic_slice_in_dim(other_half, index * rows, rows, 0)
        own, other = lax.optimization_barrier((own, other))
        return own.astype(jnp.float32) + swap(other).astype(jnp.float32)

    inward = both([(0, 1), (3, 2)])
    near_moves = both([(0, 1), (1, 0), (2, 3), (3, 2)])
    last = block(3)
    last_in = send(last.astype(bf16), inward)
    following = block(2)
    following_in = send(following.astype(bf16), inward)
    away = block(1 - inner).astype(bf16)
    away_in = send(away, near_moves)
    mine = block(inner)
    last = (last + last_in.astype(jnp.float32)).astype(bf16)
    last = send(last, both([(1, 3), (2, 0)]))
    following = (following + following_in.astype(jnp.float32)).astype(bf16)
    following = send(following, both([(1, 2), (2, 1)]))
    return mine, away_in, following, last


def sequence_end(mine, away_in, following, last):
    place = lax.axis_index("head")
    inner = (place == 1) | (place == 2)
    mine = mine + away_in.astype(jnp.float32)
    far = jnp.where(inner, following, last).astype(jnp.float32)
    keeps = lax.axis_index("pair") == place // 2
    kept = jnp.where(keeps, mine, far)
    given = jnp.where(keeps, far, mine).astype(jnp.bfloat16)
    given = swap(given)
    given = given.astype(jnp.float32)
    return in_order(kept, given, 1)


def group_moves(k):
    moves = []
    for p in range(2):
        for z in range(HEADS):
            group = 2 * (z % 2) + p
            moves.append(((p, z), (z // 2, (group + k) % HEADS)))
    return moves


def column_moves(k):
    moves = []
    for p in range(2):
        for group in range(HEADS):
            moves.append(((p, group), (group % 2, group // 2 + 2 * (p ^ k))))
    return moves


def turned(moves):
    return [(b, a) for a, b in moves]


def group_to_rows(values):
    rows = values.shape[0] // HEADS
    group = 2 * (lax.axis_index("head") % 2) + lax.axis_index("pair")
    parts = []
    for k in range(HEADS):
        start = (group + k) % HEADS * rows
        parts.append(send(lax.dynamic_slice_in_dim(values, start, rows, 0), group_moves(k)))
    return jnp.concatenate(parts, axis=1)


def rows_to_group(values):
    odd = lax.axis_index("pair") == 1
    upper = lax.axis_index("head") % 2 == 1
    parts = [
        send(part, turned(group_moves(k)))
        for k, part in enumerate(jnp.split(values, HEADS, axis=1))
    ]
    parts = [jnp.where(odd, parts[k - 1], parts[k]) for k in range(HEADS)]
    return jnp.concatenate(
        [jnp.where(upper, parts[k - 2], parts[k]) for k in range(HEADS)], axis=0
    )


def sum_all(values):
    for axis in ALL:
        size = lax.axis_size(axis)
        step = 1
        while step < size:
            values = values + lax.ppermute(values, axis, [(i, i ^ step) for i in range(size)])
            step *= 2
    return values


def layer(
    tokens, cotangent, w_query, w_key, w_value, w_out, w_up, w_down, norm_gain, norm_bias
):
    rows = tokens.shape[0]
    width = w_query.shape[1]
    model = w_query.shape[0] * lax.axis_size("outer") * 2
    bf16 = jnp.bfloat16
    f32 = jnp.float32
    late = lax.axis_index("head") // 2
    residual = tokens.astype(f32)
    norm_a, unit_a, inv_a = normalize(residual, norm_gain[0], norm_bias[0])

    w_cols = jnp.concatenate([w_query, w_key, w_value], axis=1)
    w_first, w_second = (send(w_cols, column_moves(k)) for k in range(2))
    w_cols = jnp.where(
        late == 0,
        jnp.concatenate([w_first, w_second], axis=0),
        jnp.concatenate([w_second, w_first], axis=0),
    )
    out_parts = spread(w_out.T)
    out_low = jnp.concatenate(out_parts[: HEADS // 2], axis=1)
    out_high = jnp.concatenate(out_parts[HEADS // 2 :], axis=1)
    attention = jnp.concatenate(
        [w_cols, jnp.concatenate([out_low, out_high], axis=0)], axis=1
    )
    attention = lax.all_gather(attention, "outer", axis=0, tiled=True)
    w_cols = attention[:, : 3 * width]
    out_own = attention[:, 3 * width :].reshape(-1, 2, w_out.shape[1], 2 * width)
    out_own = jnp.concatenate([out_own[:, 0], out_own[:, 1]], axis=2)
    seq_a = sequence_rows(norm_a.astype(bf16))
    up_block = half_rows(w_up)
    up_parts = spread(up_block)
    up_parts = jnp.concatenate(up_parts, axis=1)
    full_up = lax.all_gather(up_parts, "outer", axis=0, tiled=True)
    down_block = half_rows(w_down.T)
    down_parts = spread(down_block)

    block_rows = min(512, seq_a.shape[0])
    qkv = jnp.dot(seq_a, w_cols, preferred_element_type=f32).astype(bf16)
    down_parts = jnp.concatenate(down_parts, axis=1)
    full_down = lax.all_gather(down_parts, "outer", axis=0, tiled=True)
    turned_kv = qkv[:, width:].T
    seen, totals = attend(qkv, turned_kv, block_rows)
    attended = group_to_rows(seen)
    out_other = swap(out_own)
    place = lax.axis_index("pair")
    full_o = jnp.stack(
        [jnp.where(place == 0, out_own, out_other), jnp.where(place == 0, out_other, out_own)],
        axis=1,
    ).reshape(model, -1)
    mixed = contract_cols(attended, full_o)
    norm_z, unit_z, inv_z = normalize(mixed, norm_gain[1], norm_bias[1])
    hidden = residual + norm_z
    norm_c, unit_c, inv_c = normalize(hidden, norm_gain[2], norm_bias[2])
    rows_c = norm_c.astype(bf16)
    pair_c = jnp.concatenate([rows_c, swap(rows_c)], axis=0)
    pre_act = jnp.dot(pair_c, full_up, preferred_element_type=f32)
    active, gelu_back = jax.vjp(jax.nn.gelu, pre_act)
    active = active.astype(bf16)
    both_m = contract_cols(active, full_down)
    output = both_m[:rows] + swap(both_m[rows:].astype(bf16)).astype(f32)
    norm_m, unit_m, inv_m = normalize(output, norm_gain[3], norm_bias[3])
    block_out = (hidden + norm_m).astype(bf16)

    grad_y = cotangent.astype(f32)
    grad_m, gain_m, bias_m = normalize_back(grad_y, unit_m, inv_m, norm_gain[3])
    rows_gm = grad_m.astype(bf16)
    pair_gm = jnp.concatenate([rows_gm, swap(rows_gm)], axis=0)
    grad_act = jnp.dot(pair_gm, full_down, preferred_element_type=f32)
    grad_pre = gelu_back(grad_act)[0].astype(bf16)
    both_c = contract_cols(grad_pre, full_up)
    grad_c = both_c[:rows] + swap(both_c[rows:].astype(bf16)).astype(f32)
    grad_down = contract_rows(pair_gm, active).astype(bf16)
    grad_up = contract_rows(pair_c, grad_pre).astype(bf16)
    grad_more, gain_c, bias_c = normalize_back(grad_c, unit_c, inv_c, norm_gain[2])
    grad_h = grad_y + grad_more
    grad_z, gain_z, bias_z = normalize_back(grad_h, unit_z, inv_z, norm_gain[1])
    rows_gz = grad_z.astype(bf16)
    grad_att = jnp.dot(rows_gz, full_o, preferred_element_type=f32).astype(bf16)
    grad_att = rows_to_group(grad_att)
    grad_o = contract_rows(rows_gz, attended).astype(bf16)
    grad_o = grad_o.reshape(-1, 2, w_out.shape[1], attended.shape[1])
    own_o, other_o = halves(grad_o, 1)
    grad_o = (own_o.astype(f32) + swap(other_o).astype(f32)).astype(bf16)
    grad_o = grad_o.reshape(-1, attended.shape[1])
    grad_att = after(grad_att, (grad_down, grad_up, grad_o))
    grad_down = lax.psum_scatter(grad_down, "outer", scatter_dimension=0, tiled=True)
    grad_up = lax.psum_scatter(grad_up, "outer", scatter_dimension=0, tiled=True)
    grad_qkv = attend_back(qkv, turned_kv, grad_att, seen, totals, block_rows)
    grad_down = scatter_half(grad_down).T
    grad_up = scatter_half(grad_up)
    w_own, w_other = halves(w_cols, 0)
    grad_a_other = contract_cols(grad_qkv, w_other).astype(bf16)
    grad_a_own = contract_cols(grad_qkv, w_own).astype(bf16)
    grad_w = contract_rows(seq_a, after(grad_qkv, grad_a_own)).astype(bf16)
    grad_a = sequence_sum(grad_a_own, grad_a_other)
    grad_o = grad_o.reshape(-1, 1, w_out.shape[1], attended.shape[1])
    grad_o = jnp.concatenate(jnp.split(grad_o, 2, axis=3), axis=1).reshape(model, -1)
    grad_w = jnp.concatenate([grad_w, grad_o], axis=1)
    grad_w = lax.psum_scatter(grad_w, "outer", scatter_dimension=0, tiled=True)
    landed = grad_w
    grad_w, grad_o = grad_w[:, : 3 * width], grad_w[:, 3 * width :]
    grad_o = collect(
        [
            grad_o[i * w_out.shape[1] : (i + 1) * w_out.shape[1], j * width : (j + 1) * width]
            for i in range(2)
            for j in range(2)
        ]
    ).T
    size = grad_w.shape[0] // 2
    parts = [
        send(
            lax.dynamic_slice_in_dim(grad_w, jnp.where(late == k, 0, size), size, 0),
            turned(column_moves(k)),
        ).astype(f32)
        for k in range(2)
    ]
    grad_w = parts[0] + parts[1]
    grad_a = sequence_end(*grad_a[:2], *after(grad_a[2:], landed))
    grad_first, gain_a, bias_a = normalize_back(grad_a, unit_a, inv_a, norm_gain[0])
    input_grad = grad_h + grad_first
    sums = sum_all(jnp.stack([gain_a, gain_z, gain_c, gain_m, bias_a, bias_z, bias_c, bias_m]))
    return (
        block_out,
        input_grad,
        grad_w[:, :width],
        grad_w[:, width : 2 * width],
        grad_w[:, 2 * width :],
        grad_o,
        grad_up,
        grad_down,
        sums[:4],
        sums[4:],
    )


def solution(mesh):
    wide, head = mesh.shape["wide"], mesh.shape["head"]
    assert head == HEADS and wide % 2 == 0
    paired = Mesh(mesh.devices.reshape(wide // 2, 2, head), ALL)
    rows = P(ALL, None)
    by_rows = P(WIDE, "head")
    by_cols = P("head", WIDE)
    in_specs = (rows, rows, by_rows, by_rows, by_rows, by_cols, by_rows, by_cols, P(), P())
    out_specs = (rows, rows, by_rows, by_rows, by_rows, by_cols, by_rows, by_cols, P(), P())
    return jax.shard_map(
        layer, mesh=paired, in_specs=in_specs, out_specs=out_specs, check_vma=False
    )
```

```python
import math

import jax
import jax.numpy as jnp
from jax import lax
from jax.experimental import pallas as pl
from jax.experimental.pallas import tpu as pltpu
from jax.sharding import Mesh, PartitionSpec as P


HD = 64


EPS = 1e-05


def normalize(values, gain, bias):
    average = jnp.mean(values, axis=-1, keepdims=True)
    centred = values - average
    inverse = lax.rsqrt(jnp.mean(centred * centred, axis=-1, keepdims=True) + EPS)
    unit_rows = centred * inverse
    return (unit_rows * gain + bias, unit_rows, inverse)


def normalize_back(gradient, unit_rows, inverse, gain):
    scaled = gradient * gain
    inner_sum = (
        scaled
        - jnp.mean(scaled, axis=-1, keepdims=True)
        - unit_rows * jnp.mean(scaled * unit_rows, axis=-1, keepdims=True)
    )
    return (inner_sum * inverse, jnp.sum(gradient * unit_rows, axis=0), jnp.sum(gradient, axis=0))


def head_lanes(shape, head):
    lane = lax.broadcasted_iota(jnp.int32, shape, 1)
    return (lane >= head * HD) & (lane < (head + 1) * HD)


def causal(shape):
    key = lax.broadcasted_iota(jnp.int32, shape, 0)
    query = lax.broadcasted_iota(jnp.int32, shape, 1)
    return key <= query


NT = (((1,), (1,)), ((), ()))


def attend_kernel(q_ref, k_ref, vt_ref, out_ref, total_ref, acc_ref):
    block, width = q_ref.shape
    position = pl.program_id(0)
    scaled = q_ref[...] * jnp.asarray(1.0 / math.sqrt(HD), jnp.bfloat16)
    heads = [
        jnp.where(head_lanes((block, width), h), scaled, jnp.zeros_like(scaled))
        for h in range(width // HD)
    ]

    def scores(h, j):
        start = pl.multiple_of(j * block, block)
        keys = k_ref[pl.ds(start, block), :]
        return lax.dot_general(keys, heads[h], NT, preferred_element_type=jnp.float32)

    def mix(h, j, weights):
        start = pl.multiple_of(j * block, block)
        values = vt_ref[h * HD : (h + 1) * HD, pl.ds(start, block)]
        return jnp.dot(values, weights.astype(jnp.bfloat16), preferred_element_type=jnp.float32)

    first = []
    for h in range(width // HD):
        s = jnp.where(causal((block, block)), scores(h, position), -1e30)
        top = jnp.max(s, axis=0, keepdims=True)
        p = jnp.exp(s - top)
        first += [top, jnp.sum(p, axis=0, keepdims=True)]
        acc_ref[h * HD : (h + 1) * HD, :] = mix(h, position, p)

    def step(j, carry):
        carry = list(carry)
        for h in range(width // HD):
            s = scores(h, j)
            top = jnp.maximum(carry[2 * h], jnp.max(s, axis=0, keepdims=True))
            p = jnp.exp(s - top)
            old = jnp.exp(carry[2 * h] - top)
            carry[2 * h + 1] = carry[2 * h + 1] * old + jnp.sum(p, axis=0, keepdims=True)
            carry[2 * h] = top
            rows = slice(h * HD, (h + 1) * HD)
            acc_ref[rows, :] = acc_ref[rows, :] * old + mix(h, j, p)
        return tuple(carry)

    last = lax.fori_loop(0, position, step, tuple(first))
    for h in range(width // HD):
        rows = slice(h * HD, (h + 1) * HD)
        acc_ref[rows, :] = acc_ref[rows, :] / last[2 * h + 1]
        total_ref[h : h + 1, :] = last[2 * h] + jnp.log(last[2 * h + 1])
    out_ref[...] = acc_ref[...].T.astype(jnp.bfloat16)


def attend(qkv, turned_kv, block):
    length, width = qkv.shape[0], qkv.shape[1] // 3
    return pl.pallas_call(
        attend_kernel,
        grid=(length // block,),
        in_specs=[
            pl.BlockSpec((block, width), lambda i: (i, 0)),
            pl.BlockSpec((length, width), lambda i: (0, 1)),
            pl.BlockSpec((width, length), lambda i: (1, 0)),
        ],
        out_specs=[
            pl.BlockSpec((block, width), lambda i: (i, 0)),
            pl.BlockSpec((width // HD, block), lambda i: (0, i)),
        ],
        out_shape=[
            jax.ShapeDtypeStruct((length, width), jnp.bfloat16),
            jax.ShapeDtypeStruct((width // HD, length), jnp.float32),
        ],
        scratch_shapes=[pltpu.VMEM((width, block), jnp.float32)],
        name="attend",
    )(qkv, qkv, turned_kv)


def attend_back_kernel(
    q_ref, k_ref, v_ref, kt_ref, grad_ref, out_ref, total_ref, back_ref, dq_ref, dk_ref, dv_ref
):
    block, width = q_ref.shape
    position = pl.program_id(0)
    score_scale = 1.0 / math.sqrt(HD)

    @pl.when(position == 0)
    def _():
        dk_ref[...] = jnp.zeros_like(dk_ref)
        dv_ref[...] = jnp.zeros_like(dv_ref)

    dq_ref[...] = jnp.zeros_like(dq_ref)
    scaled = q_ref[...] * jnp.asarray(score_scale, jnp.bfloat16)
    grads = grad_ref[...]
    zero = jnp.zeros_like(scaled)
    query_heads = [
        jnp.where(head_lanes((block, width), h), scaled, zero) for h in range(width // HD)
    ]
    grad_heads = [
        jnp.where(head_lanes((block, width), h), grads, zero) for h in range(width // HD)
    ]
    shared = (grads.astype(jnp.float32) * out_ref[...].astype(jnp.float32)).T
    inner = [
        jnp.sum(shared[h * HD : (h + 1) * HD, :], axis=0, keepdims=True)
        for h in range(width // HD)
    ]

    def chunk(j, masked):
        rows = pl.ds(pl.multiple_of(j * block, block), block)
        keys = k_ref[rows, :]
        values = v_ref[rows, :]
        dk = dk_ref[rows, :]
        dv = dv_ref[rows, :]
        for h in range(width // HD):
            s = lax.dot_general(keys, query_heads[h], NT, preferred_element_type=jnp.float32)
            p = jnp.exp(s - total_ref[h : h + 1, :])
            if masked:
                p = jnp.where(causal((block, block)), p, 0.0)
            dp = lax.dot_general(values, grad_heads[h], NT, preferred_element_type=jnp.float32)
            ds = (p * (dp - inner[h])).astype(jnp.bfloat16)
            dv += jnp.dot(
                p.astype(jnp.bfloat16), grad_heads[h], preferred_element_type=jnp.float32
            )
            dk += jnp.dot(ds, query_heads[h], preferred_element_type=jnp.float32)
            lanes = slice(h * HD, (h + 1) * HD)
            dq_ref[lanes, :] += jnp.dot(
                kt_ref[lanes, rows], ds, preferred_element_type=jnp.float32
            )
        dk_ref[rows, :] = dk
        dv_ref[rows, :] = dv

    def step(j, carry):
        chunk(j, False)
        return carry

    lax.fori_loop(0, position, step, 0)
    chunk(position, True)
    rows = pl.ds(pl.multiple_of(position * block, block), block)
    back_ref[rows, :width] = (dq_ref[...] * score_scale).T.astype(jnp.bfloat16)

    @pl.when(position == pl.num_programs(0) - 1)
    def _():
        back_ref[:, width : 2 * width] = dk_ref[...].astype(jnp.bfloat16)
        back_ref[:, 2 * width :] = dv_ref[...].astype(jnp.bfloat16)


def attend_back(qkv, turned_kv, grad_rows, attended, totals, block):
    length, width = grad_rows.shape
    return pl.pallas_call(
        attend_back_kernel,
        grid=(length // block,),
        in_specs=[
            pl.BlockSpec((block, width), lambda i: (i, 0)),
            pl.BlockSpec((length, width), lambda i: (0, 1)),
            pl.BlockSpec((length, width), lambda i: (0, 2)),
            pl.BlockSpec((width, length), lambda i: (0, 0)),
            pl.BlockSpec((block, width), lambda i: (i, 0)),
            pl.BlockSpec((block, width), lambda i: (i, 0)),
            pl.BlockSpec((width // HD, block), lambda i: (0, i)),
        ],
        out_specs=pl.BlockSpec((length, 3 * width), lambda i: (0, 0)),
        out_shape=jax.ShapeDtypeStruct((length, 3 * width), jnp.bfloat16),
        scratch_shapes=[
            pltpu.VMEM((width, block), jnp.float32),
            pltpu.VMEM((length, width), jnp.float32),
            pltpu.VMEM((length, width), jnp.float32),
        ],
        name="attend_back",
    )(qkv, qkv, qkv, turned_kv, grad_rows, attended, totals)


def contract_rows(left_op, right_op):
    return lax.dot_general(
        left_op, right_op, (((0,), (0,)), ((), ())), preferred_element_type=jnp.float32
    )


def contract_cols(left_op, right_op):
    return lax.dot_general(
        left_op, right_op, (((1,), (1,)), ((), ())), preferred_element_type=jnp.float32
    )


WIDE = ("outer", "pair")
ALL = ("outer", "pair", "head")
LINE = ("pair", "head")
HEADS = 4


def swap(values):
    return lax.ppermute(values, "pair", [(0, 1), (1, 0)])


def send(values, moves):
    return lax.ppermute(values, LINE, [(a * HEADS + b, c * HEADS + d) for (a, b), (c, d) in moves])


def both(moves):
    return [((p, a), (p, b)) for p in range(2) for a, b in moves]


def shift(values, step):
    return lax.ppermute(values, "head", [(i, (i + step) % HEADS) for i in range(HEADS)])


def halves(block, axis):
    size = block.shape[axis] // 2
    place = lax.axis_index("pair")
    own = lax.dynamic_slice_in_dim(block, place * size, size, axis)
    other = lax.dynamic_slice_in_dim(block, (1 - place) * size, size, axis)
    return own, other


def in_order(own, other, axis):
    place = lax.axis_index("pair")
    return jnp.where(
        place == 0,
        jnp.concatenate([own, other], axis=axis),
        jnp.concatenate([other, own], axis=axis),
    )


def after(values, earlier):
    return lax.optimization_barrier((values, earlier))[0]


def spread(block):
    return [block] + [shift(block, k) for k in range(1, HEADS)]


def collect(blocks):
    total = blocks[0].astype(jnp.float32)
    for k in range(1, HEADS):
        total = total + shift(blocks[k], -k).astype(jnp.float32)
    return total


def half_rows(block):
    own, other = halves(block, 1)
    other = swap(other)
    return in_order(own, other, 0)


def scatter_half(rows):
    block = collect(jnp.split(rows, HEADS, axis=1)).astype(jnp.bfloat16)
    own, other = halves(block, 0)
    return in_order(own, swap(other), 1).astype(jnp.float32)


FORWARD = [((z // 2, z), (1 - z // 2, z)) for z in range(HEADS)]


def sequence_rows(block):
    place = lax.axis_index("head")
    holds = lax.axis_index("pair") == place // 2
    inner = (place == 1) | (place == 2)
    near = send(
        block,
        [((0, 0), (0, 1)), ((0, 1), (0, 0)), ((1, 2), (1, 3)), ((1, 3), (1, 2))],
    )
    next_in = send(block, [((0, 2), (0, 1)), ((1, 1), (1, 2))])
    last_in = send(block, [((0, 3), (0, 1)), ((1, 0), (1, 2))])
    outward = [((0, 1), (0, 0)), ((1, 2), (1, 3))]
    next_out = send(next_in, outward)
    last_out = send(last_in, outward)
    pieces = (
        block,
        near,
        jnp.where(inner, next_in, next_out),
        jnp.where(inner, last_in, last_out),
    )
    passed = [send(v, FORWARD) for v in pieces]
    own, near, following, last = (jnp.where(holds, v, w) for v, w in zip(pieces, passed))
    first = jnp.where(place % 2 == 0, own, near)
    second = jnp.where(place % 2 == 0, near, own)
    low = place < 2
    joined = jnp.concatenate(
        [
            jnp.where(low, first, last),
            jnp.where(low, second, following),
            jnp.where(low, following, first),
            jnp.where(low, last, second),
        ],
        axis=0,
    )
    return joined


def sequence_sum(own_half, other_half):
    place = lax.axis_index("head")
    low = place < 2
    inner = jnp.where((place == 1) | (place == 2), 1, 0)
    rows = own_half.shape[0] // HEADS
    bf16 = jnp.bfloat16

    def block(i):
        index = jnp.where(low, i, HEADS - 1 - i)
        own = lax.dynamic_slice_in_dim(own_half, index * rows, rows, 0)
        other = lax.dynamic_slice_in_dim(other_half, index * rows, rows, 0)
        own, other = lax.optimization_barrier((own, other))
        return own.astype(jnp.float32) + swap(other).astype(jnp.float32)

    inward = both([(0, 1), (3, 2)])
    near_moves = both([(0, 1), (1, 0), (2, 3), (3, 2)])
    last = block(3)
    last_in = send(last.astype(bf16), inward)
    following = block(2)
    following_in = send(following.astype(bf16), inward)
    away = block(1 - inner).astype(bf16)
    away_in = send(away, near_moves)
    mine = block(inner)
    last = (last + last_in.astype(jnp.float32)).astype(bf16)
    last = send(last, both([(1, 3), (2, 0)]))
    following = (following + following_in.astype(jnp.float32)).astype(bf16)
    following = send(following, both([(1, 2), (2, 1)]))
    return mine, away_in, following, last


def sequence_end(mine, away_in, following, last):
    place = lax.axis_index("head")
    inner = (place == 1) | (place == 2)
    mine = mine + away_in.astype(jnp.float32)
    far = jnp.where(inner, following, last).astype(jnp.float32)
    keeps = lax.axis_index("pair") == place // 2
    kept = jnp.where(keeps, mine, far)
    given = jnp.where(keeps, far, mine).astype(jnp.bfloat16)
    given = swap(given)
    given = given.astype(jnp.float32)
    return in_order(kept, given, 1)


def group_moves(k):
    moves = []
    for p in range(2):
        for z in range(HEADS):
            group = 2 * (z % 2) + p
            moves.append(((p, z), (z // 2, (group + k) % HEADS)))
    return moves


def column_moves(k):
    moves = []
    for p in range(2):
        for group in range(HEADS):
            moves.append(((p, group), (group % 2, group // 2 + 2 * (p ^ k))))
    return moves


def turned(moves):
    return [(b, a) for a, b in moves]


def group_to_rows(values):
    rows = values.shape[0] // HEADS
    group = 2 * (lax.axis_index("head") % 2) + lax.axis_index("pair")
    parts = []
    for k in range(HEADS):
        start = (group + k) % HEADS * rows
        parts.append(send(lax.dynamic_slice_in_dim(values, start, rows, 0), group_moves(k)))
    return jnp.concatenate(parts, axis=1)


def rows_to_group(values):
    odd = lax.axis_index("pair") == 1
    upper = lax.axis_index("head") % 2 == 1
    parts = [
        send(part, turned(group_moves(k)))
        for k, part in enumerate(jnp.split(values, HEADS, axis=1))
    ]
    parts = [jnp.where(odd, parts[k - 1], parts[k]) for k in range(HEADS)]
    return jnp.concatenate(
        [jnp.where(upper, parts[k - 2], parts[k]) for k in range(HEADS)], axis=0
    )


def sum_all(values):
    for axis in ALL:
        size = lax.axis_size(axis)
        step = 1
        while step < size:
            values = values + lax.ppermute(values, axis, [(i, i ^ step) for i in range(size)])
            step *= 2
    return values


def layer(
    tokens, cotangent, w_query, w_key, w_value, w_out, w_up, w_down, norm_gain, norm_bias
):
    rows = tokens.shape[0]
    width = w_query.shape[1]
    model = w_query.shape[0] * lax.axis_size("outer") * 2
    bf16 = jnp.bfloat16
    f32 = jnp.float32
    late = lax.axis_index("head") // 2
    residual = tokens.astype(f32)
    norm_a, unit_a, inv_a = normalize(residual, norm_gain[0], norm_bias[0])

    w_cols = jnp.concatenate([w_query, w_key, w_value], axis=1)
    w_first, w_second = (send(w_cols, column_moves(k)) for k in range(2))
    w_cols = jnp.where(
        late == 0,
        jnp.concatenate([w_first, w_second], axis=0),
        jnp.concatenate([w_second, w_first], axis=0),
    )
    out_parts = spread(w_out.T)
    out_low = jnp.concatenate(out_parts[: HEADS // 2], axis=1)
    out_high = jnp.concatenate(out_parts[HEADS // 2 :], axis=1)
    attention = jnp.concatenate(
        [w_cols, jnp.concatenate([out_low, out_high], axis=0)], axis=1
    )
    attention = lax.all_gather(attention, "outer", axis=0, tiled=True)
    w_cols = attention[:, : 3 * width]
    out_own = attention[:, 3 * width :].reshape(-1, 2, w_out.shape[1], 2 * width)
    out_own = jnp.concatenate([out_own[:, 0], out_own[:, 1]], axis=2)
    seq_a = sequence_rows(norm_a.astype(bf16))
    up_block = half_rows(w_up)
    up_parts = spread(up_block)
    up_parts = jnp.concatenate(up_parts, axis=1)
    full_up = lax.all_gather(up_parts, "outer", axis=0, tiled=True)
    down_block = half_rows(w_down.T)
    down_parts = spread(down_block)

    block_rows = min(512, seq_a.shape[0])
    qkv = jnp.dot(seq_a, w_cols, preferred_element_type=f32).astype(bf16)
    down_parts = jnp.concatenate(down_parts, axis=1)
    full_down = lax.all_gather(down_parts, "outer", axis=0, tiled=True)
    turned_kv = qkv[:, width:].T
    seen, totals = attend(qkv, turned_kv, block_rows)
    attended = group_to_rows(seen)
    out_other = swap(out_own)
    place = lax.axis_index("pair")
    full_o = jnp.stack(
        [jnp.where(place == 0, out_own, out_other), jnp.where(place == 0, out_other, out_own)],
        axis=1,
    ).reshape(model, -1)
    mixed = contract_cols(attended, full_o)
    norm_z, unit_z, inv_z = normalize(mixed, norm_gain[1], norm_bias[1])
    hidden = residual + norm_z
    norm_c, unit_c, inv_c = normalize(hidden, norm_gain[2], norm_bias[2])
    rows_c = norm_c.astype(bf16)
    pair_c = jnp.concatenate([rows_c, swap(rows_c)], axis=0)
    pre_act = jnp.dot(pair_c, full_up, preferred_element_type=f32)
    active, gelu_back = jax.vjp(jax.nn.gelu, pre_act)
    active = active.astype(bf16)
    both_m = contract_cols(active, full_down)
    output = both_m[:rows] + swap(both_m[rows:].astype(bf16)).astype(f32)
    norm_m, unit_m, inv_m = normalize(output, norm_gain[3], norm_bias[3])
    block_out = (hidden + norm_m).astype(bf16)

    grad_y = cotangent.astype(f32)
    grad_m, gain_m, bias_m = normalize_back(grad_y, unit_m, inv_m, norm_gain[3])
    rows_gm = grad_m.astype(bf16)
    pair_gm = jnp.concatenate([rows_gm, swap(rows_gm)], axis=0)
    grad_act = jnp.dot(pair_gm, full_down, preferred_element_type=f32)
    grad_pre = gelu_back(grad_act)[0].astype(bf16)
    both_c = contract_cols(grad_pre, full_up)
    grad_c = both_c[:rows] + swap(both_c[rows:].astype(bf16)).astype(f32)
    grad_down = contract_rows(pair_gm, active).astype(bf16)
    grad_up = contract_rows(pair_c, grad_pre).astype(bf16)
    grad_more, gain_c, bias_c = normalize_back(grad_c, unit_c, inv_c, norm_gain[2])
    grad_h = grad_y + grad_more
    grad_z, gain_z, bias_z = normalize_back(grad_h, unit_z, inv_z, norm_gain[1])
    rows_gz = grad_z.astype(bf16)
    grad_att = jnp.dot(rows_gz, full_o, preferred_element_type=f32).astype(bf16)
    grad_att = rows_to_group(grad_att)
    grad_o = contract_rows(rows_gz, attended).astype(bf16)
    grad_o = grad_o.reshape(-1, 2, w_out.shape[1], attended.shape[1])
    own_o, other_o = halves(grad_o, 1)
    grad_o = (own_o.astype(f32) + swap(other_o).astype(f32)).astype(bf16)
    grad_o = grad_o.reshape(-1, attended.shape[1])
    grad_att = after(grad_att, (grad_down, grad_up, grad_o))
    grad_down = lax.psum_scatter(grad_down, "outer", scatter_dimension=0, tiled=True)
    grad_up = lax.psum_scatter(grad_up, "outer", scatter_dimension=0, tiled=True)
    grad_qkv = attend_back(qkv, turned_kv, grad_att, seen, totals, block_rows)
    grad_down = scatter_half(grad_down).T
    grad_up = scatter_half(grad_up)
    w_own, w_other = halves(w_cols, 0)
    grad_a_other = contract_cols(grad_qkv, w_other).astype(bf16)
    grad_a_own = contract_cols(grad_qkv, w_own).astype(bf16)
    grad_w = contract_rows(seq_a, grad_qkv).astype(bf16)
    grad_a = sequence_sum(grad_a_own, grad_a_other)
    grad_o = grad_o.reshape(-1, 1, w_out.shape[1], attended.shape[1])
    grad_o = jnp.concatenate(jnp.split(grad_o, 2, axis=3), axis=1).reshape(model, -1)
    grad_w = jnp.concatenate([grad_w, grad_o], axis=1)
    grad_w = lax.psum_scatter(grad_w, "outer", scatter_dimension=0, tiled=True)
    landed = grad_w
    grad_w, grad_o = grad_w[:, : 3 * width], grad_w[:, 3 * width :]
    grad_o = [
        grad_o[i * w_out.shape[1] : (i + 1) * w_out.shape[1], j * width : (j + 1) * width]
        for i in range(2)
        for j in range(2)
    ]
    grad_o = collect(grad_o).T
    size = grad_w.shape[0] // 2
    parts = [
        send(
            lax.dynamic_slice_in_dim(grad_w, jnp.where(late == k, 0, size), size, 0),
            turned(column_moves(k)),
        ).astype(f32)
        for k in range(2)
    ]
    grad_w = parts[0] + parts[1]
    grad_a = sequence_end(*grad_a[:2], *after(grad_a[2:], landed))
    grad_first, gain_a, bias_a = normalize_back(grad_a, unit_a, inv_a, norm_gain[0])
    input_grad = grad_h + grad_first
    sums = sum_all(jnp.stack([gain_a, gain_z, gain_c, gain_m, bias_a, bias_z, bias_c, bias_m]))
    return (
        block_out,
        input_grad,
        grad_w[:, :width],
        grad_w[:, width : 2 * width],
        grad_w[:, 2 * width :],
        grad_o,
        grad_up,
        grad_down,
        sums[:4],
        sums[4:],
    )


def solution(mesh):
    wide, head = mesh.shape["wide"], mesh.shape["head"]
    assert head == HEADS and wide % 2 == 0
    paired = Mesh(mesh.devices.reshape(wide // 2, 2, head), ALL)
    rows = P(ALL, None)
    by_rows = P(WIDE, "head")
    by_cols = P("head", WIDE)
    in_specs = (rows, rows, by_rows, by_rows, by_rows, by_cols, by_rows, by_cols, P(), P())
    out_specs = (rows, rows, by_rows, by_rows, by_rows, by_cols, by_rows, by_cols, P(), P())
    return jax.shard_map(
        layer, mesh=paired, in_specs=in_specs, out_specs=out_specs, check_vma=False
    )
```
